32 devices in a mesh: groups: 2 (over x), wide: 8 (over z, y), narrow: 2 (over core).
Axes of the slice: x: 2, y: 2, z: 4, core: 2. Of those that a mesh axis runs over, the one named last changes fastest.
Arguments:
- tokens: bfloat16 [4096, 4096], P(('groups', 'wide')), parts along dimension 0, may hold values from -6 to 6
- norm_gain: float32 [4096], replicated, may hold values from 0.1 to 1.9
- w_in: bfloat16 [4096, 1024], P('wide'), may hold values from -0.09375 to 0.09375
- w_out: bfloat16 [1024, 4096], P('wide', 'narrow'), may hold values from -0.1875 to 0.1875
- w_up: bfloat16 [8, 1024, 2688], P('wide', None, 'narrow'), may hold values from -0.1875 to 0.1875
- w_down: bfloat16 [8, 2688, 1024], P('wide', 'narrow'), may hold values from -0.15625 to 0.15625
- expert_ids: int32 [4096, 4], P(('groups', 'wide')), parts along dimension 0, may hold values from 0 to 7, all different within a row; in each aligned block of 256 rows (0 to 255, 256 to 511, ...) at most 192 rows name the same one
- gate_weights: float32 [4096, 4], P(('groups', 'wide')), parts along dimension 0, may hold values from 0.1 to 1
Outputs:
- result: bfloat16 [4096, 4096], P(('groups', 'wide'), 'narrow'), parts along dimension 0
The draws below stay inside these ranges and needn't reach their ends.
There are 2 independent parts, one for each index of `groups`. The reference program is written for one: setup_inputs(seed, part) draws one part's arguments, and reference() takes and returns one part's arrays. A program takes and returns all parts, laid end to end along the dimension named above; an argument that names none is the same for every part. Nothing has to cross between parts.
Inputs may be any that keep to these rules, and one draw needn't show every extreme that they name: `expert_ids`: within the 256 rows of one index of wide, the entries of a row differ and no expert is named by more than 192 rows.
All inputs are finite; a program needn't handle non-finite values.
Results may differ from the reference program's by a relative error of at most 0.013.
Values may be sent and summed in bfloat16 or wider, within the bound.
A program may use at most 128 MiB of HBM per device.

```python
import math
import jax
import jax.numpy as jnp
import numpy as np
from jax import lax

D = 4096
L = 1024
HID = 2688
TOPK = 4
TOK_DEV = 256
EXPERTS = 8
CAP = 192
TOKENS = 2048


def level_of(rng, dims, cuts, low, largest):
    def one(axis_at, parts):
        steps = jax.random.uniform(jax.random.fold_in(jax.random.fold_in(rng, 6), axis_at), (parts,), jnp.float32, low / len(cuts), largest / len(cuts))
        return jnp.repeat(jnp.exp(steps), dims[axis_at] // parts).reshape((-1,) + (1,) * (len(dims) - axis_at - 1))

    gain = one(*cuts[0])
    for cut in cuts[1:]:
        gain = gain * one(*cut)
    return gain


def deal_out(own_key, own, number, rows, number_of, top, limit, slope):
    order = jax.random.permutation(own_key, number_of)
    crowded, ordinary = load_shares(number_of, rows * top, limit, slope, True), load_shares(number_of, rows * top, limit, slope, False)
    places = jnp.arange(number_of)

    def named(sizes, rotation):
        used = int((sizes > 0).sum())
        fixed = max(1, used // 4)
        moved = fixed + (places - fixed + rotation * (used - fixed)) % max(1, number_of - fixed)
        return jnp.zeros((number_of,), jnp.int32).at[order[jnp.where(places < fixed, places, moved)]].set(jnp.asarray(sizes, jnp.int32))

    sizes = jnp.where(number % 4 == 0, named(crowded, number // 4), named(ordinary, number - number // 4 - 1))
    mixed = jax.random.permutation(jax.random.fold_in(own, 3), number_of)
    donor, taker = mixed[0:number_of // 2 * 2:2], mixed[1:number_of // 2 * 2:2]
    slack = jnp.minimum(sizes[donor] - 1, limit - sizes[taker]) // 2
    slack = jnp.where((donor == order[0]) | (taker == order[0]) | (sizes[taker] == 0), 0, jnp.maximum(slack, 0))
    moved = jax.random.randint(jax.random.fold_in(own, 4), (number_of // 2,), 0, 1 << 20) % (slack + 1)
    sizes = sizes.at[donor].add(-moved).at[taker].add(moved)
    items = jnp.searchsorted(jnp.cumsum(sizes), jnp.arange(rows * top), side="right").astype(jnp.int32)
    grid = items.reshape(top, rows).T
    grid = grid[jax.random.permutation(jax.random.fold_in(own, 1), rows)]
    rotation = jax.random.randint(jax.random.fold_in(own, 2), (rows, 1), 0, top)
    return jnp.take_along_axis(grid, (jnp.arange(top)[None, :] + rotation) % top, axis=1)


def load_shares(amount, total, limit, lean, full):
    weights = [(1 << 20) // math.isqrt(grade ** lean) + 1 for grade in range(1, amount + 1)]
    largest = limit if full else min(limit, max(-(-total // amount), total * weights[0] // sum(weights)))
    least = 1 if total - largest >= amount - 1 else 0
    given, spare = [largest] + [least] * (amount - 1), total - largest - least * (amount - 1)
    while spare > 0:
        candidates = [i for i in range(1, amount) if given[i] < largest] or [i for i in range(1, amount) if given[i] < limit]
        mass, budget = sum([weights[i] for i in candidates]), spare
        for i in candidates:
            more = min(limit - given[i], max(1, budget * weights[i] // mass), spare)
            given[i] = given[i] + more
            spare = spare - more
    return np.array(given)


def noise(key, shape, deviation, reach, split=(), kind=jnp.bfloat16):
    result = deviation * jax.random.normal(key, shape, jnp.float32)
    if split:
        result = result * level_of(key, shape, split, -0.22, 0.18)
    return jnp.clip(result, -reach, reach).astype(kind)


def setup_inputs(seed: int = 0, part: int = 0) -> dict:
    seeds = jax.random.split(jax.random.key(seed), 9)
    own_keys = jax.random.split(jax.random.fold_in(seeds[8], part), 9)
    tokens = noise(own_keys[0], (TOKENS, D), 1.0, 6.0, ((0, 8),))
    norm_gain = jnp.clip(1.0 + 0.18 * jax.random.normal(seeds[1], (D,), jnp.float32), 0.1, 1.9)
    w_in = noise(seeds[2], (D, L), D ** -0.5, 0.09375, ((0, 8),))
    w_out = noise(seeds[3], (L, D), L ** -0.5, 0.1875, ((0, 8), (1, 2)))
    w_up = noise(seeds[4], (EXPERTS, L, HID), L ** -0.5, 0.1875, ((0, 8), (2, 2)))
    w_down = noise(seeds[5], (EXPERTS, HID, L), (HID // 2) ** -0.5, 0.15625, ((0, 8), (1, 2)))
    expert_ids_keys = jax.random.split(jax.random.fold_in(own_keys[6], 1), TOKENS // TOK_DEV)
    expert_ids_turns = jax.random.permutation(jax.random.fold_in(own_keys[6], 3), TOKENS // TOK_DEV)
    expert_ids = jax.vmap(lambda own, number: deal_out(jax.random.fold_in(own_keys[6], 2), own, number, TOK_DEV, EXPERTS, TOPK, CAP, 1))(expert_ids_keys, expert_ids_turns).reshape((TOKENS, TOPK))
    gate_weights = jnp.clip(jnp.exp(math.log(1.0) - 2.3025851 * jax.random.uniform(own_keys[7], (TOKENS, TOPK), jnp.float32) ** level_of(own_keys[7], (TOKENS, TOPK), ((0, 8),), -0.2, 0.2)), 0.1, 1.0)
    return {"tokens": tokens, "norm_gain": norm_gain, "w_in": w_in, "w_out": w_out, "w_up": w_up, "w_down": w_down, "expert_ids": expert_ids, "gate_weights": gate_weights}


def reference(tokens, norm_gain, w_in, w_out, w_up, w_down, expert_ids, gate_weights):
    widened = tokens.astype(jnp.float32)
    scale = lax.rsqrt(lax.optimization_barrier(jnp.mean(widened * widened, axis=-1, keepdims=True)) + 1e-05)
    normed = (widened * scale * norm_gain).astype(jnp.bfloat16)
    latent = jnp.dot(normed, w_in, preferred_element_type=jnp.float32).astype(jnp.bfloat16)
    blocks = TOKENS // TOK_DEV
    per_block = expert_ids.reshape(blocks, TOK_DEV * TOPK)
    onehot = (per_block[:, :, None] == jnp.arange(EXPERTS, dtype=jnp.int32)[None, None, :]).astype(jnp.int32)
    slot_index = lax.optimization_barrier(jnp.sum((jnp.cumsum(onehot, axis=1) - 1) * onehot, axis=-1))
    block_index = jnp.arange(blocks, dtype=jnp.int32)[:, None]
    rows_expert = blocks * CAP
    target = (per_block * rows_expert + block_index * CAP + slot_index).reshape(-1).astype(jnp.int32)
    repeated = jnp.repeat(latent, TOPK, axis=0)
    inputs = jnp.zeros((EXPERTS * rows_expert, L), jnp.bfloat16).at[target].set(repeated)
    inputs = inputs.reshape(EXPERTS, rows_expert, L)

    def one_expert(packed):
        rows, up_weight, down_weight = packed
        hidden = jnp.dot(rows, up_weight, preferred_element_type=jnp.float32)
        hidden = jnp.square(jnp.maximum(hidden, 0.0)).astype(jnp.bfloat16)
        return jnp.dot(hidden, down_weight, preferred_element_type=jnp.float32).astype(jnp.bfloat16)
    outputs = lax.map(one_expert, (inputs, w_up, w_down)).reshape(EXPERTS * rows_expert, L)
    picked = outputs[target].astype(jnp.float32).reshape(TOKENS, TOPK, L)
    mixture = lax.optimization_barrier(jnp.sum(picked * gate_weights[:, :, None], axis=1)).astype(jnp.bfloat16)
    branch = jnp.dot(mixture, w_out, preferred_element_type=jnp.float32)
    return (widened + branch).astype(jnp.bfloat16)
```

```python
import functools
import jax
import jax.numpy as jnp
from jax import lax
from jax.experimental import pallas as pl
from jax.experimental.pallas import tpu as pltpu
from jax.sharding import PartitionSpec as P

F32 = jnp.float32
BF16 = jnp.bfloat16


def kernel(
    tok_hbm, gain_ref, win_hbm, wout_hbm, up_hbm, down_hbm, gates_hbm, out_ref,
    tok, nb, win, wo, up, down, gbuf, lat, acc, xsend, obuf, ownp, ysend, yrecv, zsend, zrecv, macc, mixb,
    loc, gs, gr, es, er, az_s, az_r, ay_s, ay_r, ax_s, ax_r, bz_s, bz_r, by_s, by_r, bx_s, bx_r,
    cz_s, cz_r, cy_s, cy_r, cc_s, cc_r, dy_s, dy_r, dz_s, dz_r, mc_s, mc_r,
):
    wide = lax.axis_size("wide")
    zs = wide // 2
    g, w, c = lax.axis_index("groups"), lax.axis_index("wide"), lax.axis_index("narrow")
    z, y = w // 2, w % 2
    gh = g % 2
    xpeer = {"groups": g + 1 - 2 * gh}
    ypeer = {"wide": w + 1 - 2 * y}
    cpeer = {"narrow": 1 - c}
    MESH = pl.DeviceIdType.MESH

    def zfwd(k):
        return {"wide": lax.rem(z + k, zs) * 2 + y}

    def zback(k):
        return {"wide": lax.rem(z + zs - k, zs) * 2 + y}

    def blk(k, yy):
        return lax.rem(z + zs - k, zs) * 2 + yy

    def rcopy(src, dst, ss, rs, dev):
        return pltpu.make_async_remote_copy(
            src_ref=src, dst_ref=dst, send_sem=ss, recv_sem=rs, device_id=dev, device_id_type=MESH
        )

    def loop(lo, hi, body):
        def step(i, carry):
            body(i)
            return carry

        lax.fori_loop(lo, hi, step, 0)

    half_in = win.shape[2]
    lcols = win.shape[3]
    half_out = wo.shape[2]
    tokens = tok.shape[0]
    th = lat.shape[2]
    oy = 1 - y

    in_cols = pl.ds(pl.multiple_of(c * lcols, lcols), lcols)
    lc_tok = pltpu.make_async_copy(tok_hbm, tok, loc.at[0])
    lc_in = [
        pltpu.make_async_copy(
            win_hbm.at[pl.ds(h * half_in, half_in), in_cols], win.at[w, h], loc.at[1 + h]
        )
        for h in range(2)
    ]
    lc_out = [
        pltpu.make_async_copy(wout_hbm.at[pl.ds(h * half_out, half_out), :], wo.at[w, h], loc.at[3 + h])
        for h in range(2)
    ]
    lc_up = pltpu.make_async_copy(up_hbm.at[0], up.at[c], loc.at[5])
    lc_down = pltpu.make_async_copy(down_hbm.at[0], down.at[c], loc.at[6])
    lc_g = pltpu.make_async_copy(gates_hbm.at[c], gbuf.at[w], loc.at[7])
    for cp in lc_in + [lc_tok, lc_g, lc_up, lc_down] + lc_out:
        cp.start()

    barrier = pltpu.get_barrier_semaphore()
    loop(1, wide, lambda d: pl.semaphore_signal(
        barrier, inc=1, device_id={"wide": lax.rem(w + d, wide)}, device_id_type=MESH))
    pl.semaphore_signal(barrier, inc=1, device_id=xpeer, device_id_type=MESH)
    pl.semaphore_signal(barrier, inc=1, device_id=cpeer, device_id_type=MESH)
    pl.semaphore_wait(barrier, wide + 1)

    def gather(buf, z_s, z_r, y_s, y_r, x_s, x_r):
        def zc(k):
            return rcopy(buf.at[w, gh], buf.at[w, gh], z_s.at[k], z_r.at[k], zfwd(k))

        def zw(k):
            s = buf.at[blk(k, y), gh]
            return rcopy(s, s, z_s.at[k], z_r.at[k], zfwd(k))

        def yc(k):
            s = buf.at[blk(k, y), gh]
            return rcopy(s, s, y_s.at[k], y_r.at[k], ypeer)

        def yw(k):
            s = buf.at[blk(k, oy), gh]
            return rcopy(s, s, y_s.at[k], y_r.at[k], ypeer)

        def x_copy(k, far):
            s = buf.at[blk(k, oy if far else y), gh]
            i = k + zs if far else k
            return rcopy(s, s, x_s.at[i], x_r.at[i], xpeer)

        def x_wait(k, far):
            s = buf.at[blk(k, oy if far else y), 1 - gh]
            i = k + zs if far else k
            return rcopy(s, s, x_s.at[i], x_r.at[i], xpeer)

        return zc, zw, yc, yw, x_copy, x_wait

    azc, azw, ayc, ayw, axc, axw = gather(win, az_s, az_r, ay_s, ay_r, ax_s, ax_r)
    bzc, bzw, byc, byw, bxc, bxw = gather(wo, bz_s, bz_r, by_s, by_r, bx_s, bx_r)

    lc_in[0].wait()
    lc_in[1].wait()
    loop(1, zs, lambda k: azc(k).start())
    ayc(0).start()

    e_up = rcopy(up_hbm.at[0], up.at[c], es.at[0], er.at[0], cpeer)
    e_down = rcopy(down_hbm.at[0], down.at[c], es.at[1], er.at[1], cpeer)
    e_up.start()
    e_down.start()
    lc_g.wait()

    def gcopy(d):
        return rcopy(gbuf.at[w], gbuf.at[w], gs.at[d], gr.at[d], {"wide": lax.rem(w + d, wide)})

    def gwait(d):
        s = gbuf.at[lax.rem(w + wide - d, wide)]
        return rcopy(s, s, gs.at[d], gr.at[d], {"wide": lax.rem(w + d, wide)})

    loop(1, wide, lambda d: gcopy(d).start())

    lc_tok.wait()
    step_rows = 32
    rin = nb.shape[2]

    def norm(i):
        rows = pl.ds(pl.multiple_of(i * step_rows, step_rows), step_rows)
        x = tok[rows, :].astype(F32)
        scale = lax.rsqrt(jnp.mean(x * x, axis=-1, keepdims=True) + 1e-05)
        n = (x * scale * gain_ref[...]).astype(BF16)
        for j in range(wide):
            nb[j, rows, :] = n[:, j * rin : (j + 1) * rin]

    loop(0, tokens // step_rows, norm)

    def madd(b):
        wb = win[b].reshape(2 * half_in, lcols)
        acc[...] += jnp.dot(nb[b], wb, preferred_element_type=F32)

    acc[...] = jnp.zeros_like(acc)
    madd(w)

    def z_arrive(k):
        azw(k).wait_recv()
        axc(k, False).start()
        ayc(k).start()

    ayw(0).wait_recv()
    axc(0, True).start()
    loop(1, zs, z_arrive)

    def y_arrive(k):
        ayw(k).wait_recv()
        axc(k, True).start()

    loop(1, zs, y_arrive)
    lc_out[0].wait()
    lc_out[1].wait()
    loop(1, zs, lambda k: bzc(k).start())

    def use_far(k):
        axw(k, True).wait_recv()
        madd(blk(k, oy))

    def use_near(k):
        axw(k, False).wait_recv()
        madd(blk(k, y))

    use_far(0)
    loop(1, zs, use_near)
    loop(1, zs, use_far)

    lat[w, c] = acc[pl.ds(pl.multiple_of(c * th, th), th), :].astype(BF16)
    xsend[...] = acc[pl.ds(pl.multiple_of((1 - c) * th, th), th), :].astype(BF16)
    swap = rcopy(xsend, lat.at[w, c], cc_s, cc_r, cpeer)
    swap.start()
    rcopy(xsend, lat.at[w, 1 - c], cc_s, cc_r, cpeer).wait_recv()

    def czc(k):
        return rcopy(lat.at[w], lat.at[w], cz_s.at[k], cz_r.at[k], zfwd(k))

    def czw(k):
        s = lat.at[blk(k, y)]
        return rcopy(s, s, cz_s.at[k], cz_r.at[k], zfwd(k))

    def cyc(k):
        s = lat.at[blk(k, y)]
        return rcopy(s, s, cy_s.at[k], cy_r.at[k], ypeer)

    def cyw(k):
        s = lat.at[blk(k, oy)]
        return rcopy(s, s, cy_s.at[k], cy_r.at[k], ypeer)

    cyc(0).start()
    loop(1, zs, lambda k: czc(k).start())

    lc_up.wait()
    lc_down.wait()
    rcopy(up_hbm.at[0], up.at[1 - c], es.at[0], er.at[0], cpeer).wait_recv()
    rcopy(down_hbm.at[0], down.at[1 - c], es.at[1], er.at[1], cpeer).wait_recv()
    loop(1, wide, lambda d: gwait(d).wait_recv())

    def gate_col(b):
        gt = gbuf[b]
        mine = lax.broadcasted_iota(jnp.int32, gt.shape, 0) == w
        row = jnp.sum(jnp.where(mine, gt, 0.0), axis=0, keepdims=True)
        return jnp.transpose(jnp.broadcast_to(row, (8, th)))[:, :1]

    def dyc(k):
        return rcopy(ysend.at[k], yrecv.at[k], dy_s.at[k], dy_r.at[k], ypeer)

    def dzc(k):
        return rcopy(zsend.at[k], zrecv.at[k], dz_s.at[k], dz_r.at[k], zback(k))

    def expert(k):
        b0 = blk(k, 0)
        x0 = jnp.concatenate([lat[b0, 0], lat[b0 + 1, 0]], axis=0)
        x1 = jnp.concatenate([lat[b0, 1], lat[b0 + 1, 1]], axis=0)
        x = jnp.concatenate([x0, x1], axis=1)
        total = None
        for h in range(2):
            hid = jnp.dot(x, up[h], preferred_element_type=F32)
            hid = jnp.square(jnp.maximum(hid, 0.0)).astype(BF16)
            part = jnp.dot(hid, down[h], preferred_element_type=F32)
            total = part if total is None else total + part
        obuf[0] = total[:th] * gate_col(b0)
        obuf[1] = total[th:] * gate_col(b0 + 1)
        ysend[k] = obuf[oy].astype(BF16)
        dyc(k).start()
        ownp[lax.rem(k, 2)] = obuf[y]

    def finish(k):
        dyc(k).wait_recv()
        zsend[k] = (ownp[lax.rem(k, 2)] + yrecv[k].astype(F32)).astype(BF16)
        dzc(k).start()

    def arrive(k):
        czw(k).wait_recv()
        cyc(k).start()

    loop(1, zs, arrive)
    cyw(0).wait_recv()
    expert(0)

    def b_arrive(k):
        bzw(k).wait_recv()
        bxc(k, False).start()

    loop(1, zs, b_arrive)

    def expert_step(k):
        cyw(k).wait_recv()
        expert(k)

        @pl.when(k > 1)
        def _():
            finish(k - 1)

        @pl.when(k == 1)
        def _():
            dyc(0).wait_recv()
            macc[...] = ownp[0] + yrecv[0].astype(F32)

    loop(1, zs, expert_step)
    loop(0, zs, lambda k: byc(k).start())
    finish(zs - 1)

    def by_arrive(k):
        byw(k).wait_recv()
        bxc(k, True).start()

    loop(0, zs, by_arrive)

    def collect(k):
        dzc(k).wait_recv()
        macc[...] += zrecv[k].astype(F32)

    loop(1, zs, collect)
    mixb[c] = macc[...].astype(BF16)
    mcopy = rcopy(mixb.at[c], mixb.at[c], mc_s, mc_r, cpeer)
    mcopy.start()
    rcopy(mixb.at[1 - c], mixb.at[1 - c], mc_s, mc_r, cpeer).wait_recv()
    loop(1, zs, lambda k: bxw(k, False).wait_recv())
    loop(0, zs, lambda k: bxw(k, True).wait_recv())

    ocols = out_ref.shape[1]
    width = min(512, ocols)

    def project(i):
        m = mixb[...].reshape(tokens, mixb.shape[2])
        off = pl.multiple_of(i * width, width)
        wv = wo[:, :, :, pl.ds(off, width)].reshape(mixb.shape[2], width)
        branch = jnp.dot(m, wv, preferred_element_type=F32)
        own = tok[:, pl.ds(pl.multiple_of(c * ocols + off, width), width)].astype(F32)
        out_ref[:, pl.ds(off, width)] = (own + branch).astype(out_ref.dtype)

    loop(0, ocols // width, project)

    loop(1, wide, lambda d: gcopy(d).wait_send())
    e_up.wait_send()
    e_down.wait_send()
    swap.wait_send()
    mcopy.wait_send()
    for zc, yc, xc in ((azc, ayc, axc), (bzc, byc, bxc)):
        loop(1, zs, lambda k: zc(k).wait_send())
        loop(0, zs, lambda k: yc(k).wait_send())
        loop(1, zs, lambda k: xc(k, False).wait_send())
        loop(0, zs, lambda k: xc(k, True).wait_send())
    loop(1, zs, lambda k: czc(k).wait_send())
    loop(0, zs, lambda k: cyc(k).wait_send())
    loop(0, zs, lambda k: dyc(k).wait_send())
    loop(1, zs, lambda k: dzc(k).wait_send())


def local(tokens, norm_gain, w_in, w_out, w_up, w_down, expert_ids, gate_weights):
    wide = lax.axis_size("wide")
    zs = wide // 2
    rows, depth = tokens.shape
    half = rows // 2
    latent = w_in.shape[1]
    ids = expert_ids.T
    chosen = ids[:, None, :] == jnp.arange(wide, dtype=jnp.int32)[None, :, None]
    gates = jnp.sum(jnp.where(chosen, gate_weights.T[:, None, :], 0.0), axis=0)
    gates = gates.reshape(wide, 2, half).transpose(1, 0, 2)
    any_ = pl.BlockSpec(memory_space=pl.ANY)
    vmem = pl.BlockSpec(memory_space=pltpu.VMEM)
    dma = pltpu.SemaphoreType.DMA
    hid = w_up.shape[2]
    cols = w_out.shape[1]
    V = pltpu.VMEM
    scratch = [
        V((rows, depth), BF16),
        V((wide, rows, depth // wide), BF16),
        V((wide, 2, w_in.shape[0] // 2, latent // 2), BF16),
        V((wide, 2, w_out.shape[0] // 2, cols), BF16),
        V((2, latent, hid), BF16),
        V((2, hid, latent), BF16),
        V((wide, wide, half), F32),
        V((wide, 2, half, latent // 2), BF16),
        V((rows, latent // 2), F32),
        V((half, latent // 2), BF16),
        V((2, half, latent), F32),
        V((2, half, latent), F32),
        V((zs, half, latent), BF16),
        V((zs, half, latent), BF16),
        V((zs, half, latent), BF16),
        V((zs, half, latent), BF16),
        V((half, latent), F32),
        V((2, half, latent), BF16),
        dma((8,)),
        dma((wide,)), dma((wide,)),
        dma((2,)), dma((2,)),
    ]
    scratch += [dma((zs,)), dma((zs,)), dma((zs,)), dma((zs,)), dma((wide,)), dma((wide,))] * 2
    scratch += [dma((zs,))] * 4 + [dma, dma] + [dma((zs,))] * 4 + [dma, dma]
    return pl.pallas_call(
        kernel,
        out_shape=jax.ShapeDtypeStruct((rows, cols), BF16),
        in_specs=[any_, vmem, any_, any_, any_, any_, any_],
        out_specs=vmem,
        scratch_shapes=scratch,
        compiler_params=pltpu.CompilerParams(
            collective_id=0, has_side_effects=True, vmem_limit_bytes=66_000_000
        ),
        name="moe",
    )(tokens, norm_gain.reshape(1, depth), w_in, w_out, w_up, w_down, gates)


def solution(mesh):
    in_specs = (
        P(("groups", "wide"), None),
        P(),
        P("wide", None),
        P("wide", "narrow"),
        P("wide", None, "narrow"),
        P("wide", "narrow", None),
        P(("groups", "wide"), None),
        P(("groups", "wide"), None),
    )
    out_specs = P(("groups", "wide"), "narrow")
    return jax.shard_map(local, mesh=mesh, in_specs=in_specs, out_specs=out_specs, check_vma=False)
```

```python
import functools
import jax
import jax.numpy as jnp
from jax import lax
from jax.experimental import pallas as pl
from jax.experimental.pallas import tpu as pltpu
from jax.sharding import PartitionSpec as P

F32 = jnp.float32
BF16 = jnp.bfloat16


def kernel(
    tok_hbm, gain_ref, win_hbm, wout_hbm, up_hbm, down_hbm, gates_hbm, out_ref,
    tok, nb, nby, win, wo, up, down, gbuf, lat, acc, psend, precv, xsend, obuf, ownp, ysend, yrecv, zsend, zrecv, macc, mixb,
    loc, gs, gr, es, er, az_s, az_r, ax_s, ax_r, ty_s, ty_r, tc_s, tc_r, py_s, py_r, bz_s, bz_r, by_s, by_r, bx_s, bx_r,
    cz_s, cz_r, cy_s, cy_r, cc_s, cc_r, dy_s, dy_r, dz_s, dz_r, mc_s, mc_r,
):
    wide = lax.axis_size("wide")
    zs = wide // 2
    g, w, c = lax.axis_index("groups"), lax.axis_index("wide"), lax.axis_index("narrow")
    z, y = w // 2, w % 2
    gh = g % 2
    xpeer = {"groups": g + 1 - 2 * gh}
    ypeer = {"wide": w + 1 - 2 * y}
    cpeer = {"narrow": 1 - c}
    MESH = pl.DeviceIdType.MESH

    def zfwd(k):
        return {"wide": lax.rem(z + k, zs) * 2 + y}

    def zback(k):
        return {"wide": lax.rem(z + zs - k, zs) * 2 + y}

    def blk(k, yy):
        return lax.rem(z + zs - k, zs) * 2 + yy

    def rcopy(src, dst, ss, rs, dev):
        return pltpu.make_async_remote_copy(
            src_ref=src, dst_ref=dst, send_sem=ss, recv_sem=rs, device_id=dev, device_id_type=MESH
        )

    def loop(lo, hi, body):
        def step(i, carry):
            body(i)
            return carry

        lax.fori_loop(lo, hi, step, 0)

    half_in = win.shape[2]
    lcols = win.shape[3]
    half_out = wo.shape[2]
    tokens = tok.shape[0]
    th = lat.shape[2]
    oy = 1 - y

    in_cols = pl.ds(pl.multiple_of(c * lcols, lcols), lcols)
    lc_tok = pltpu.make_async_copy(tok_hbm, tok, loc.at[0])
    lc_in = [
        pltpu.make_async_copy(
            win_hbm.at[pl.ds(h * half_in, half_in), in_cols], win.at[z, h], loc.at[1 + h]
        )
        for h in range(2)
    ]
    lc_out = [
        pltpu.make_async_copy(wout_hbm.at[pl.ds(h * half_out, half_out), :], wo.at[w, h], loc.at[3 + h])
        for h in range(2)
    ]
    lc_up = pltpu.make_async_copy(up_hbm.at[0], up.at[c], loc.at[5])
    lc_down = pltpu.make_async_copy(down_hbm.at[0], down.at[c], loc.at[6])
    lc_g = pltpu.make_async_copy(gates_hbm.at[c], gbuf.at[w], loc.at[7])
    for cp in lc_in + [lc_tok, lc_g, lc_up, lc_down] + lc_out:
        cp.start()

    barrier = pltpu.get_barrier_semaphore()
    loop(1, wide, lambda d: pl.semaphore_signal(
        barrier, inc=1, device_id={"wide": lax.rem(w + d, wide)}, device_id_type=MESH))
    pl.semaphore_signal(barrier, inc=1, device_id=xpeer, device_id_type=MESH)
    pl.semaphore_signal(barrier, inc=1, device_id=cpeer, device_id_type=MESH)
    pl.semaphore_wait(barrier, wide + 1)

    def gather(buf, z_s, z_r, y_s, y_r, x_s, x_r):
        def zc(k):
            return rcopy(buf.at[w, gh], buf.at[w, gh], z_s.at[k], z_r.at[k], zfwd(k))

        def zw(k):
            s = buf.at[blk(k, y), gh]
            return rcopy(s, s, z_s.at[k], z_r.at[k], zfwd(k))

        def yc(k):
            s = buf.at[blk(k, y), gh]
            return rcopy(s, s, y_s.at[k], y_r.at[k], ypeer)

        def yw(k):
            s = buf.at[blk(k, oy), gh]
            return rcopy(s, s, y_s.at[k], y_r.at[k], ypeer)

        def x_copy(k, far):
            s = buf.at[blk(k, oy if far else y), gh]
            i = k + zs if far else k
            return rcopy(s, s, x_s.at[i], x_r.at[i], xpeer)

        def x_wait(k, far):
            s = buf.at[blk(k, oy if far else y), 1 - gh]
            i = k + zs if far else k
            return rcopy(s, s, x_s.at[i], x_r.at[i], xpeer)

        return zc, zw, yc, yw, x_copy, x_wait

    def zback_z(k):
        return lax.rem(z + zs - k, zs)

    def azc(k):
        return rcopy(win.at[z, gh], win.at[z, gh], az_s.at[k], az_r.at[k], zfwd(k))

    def azw(k):
        s = win.at[zback_z(k), gh]
        return rcopy(s, s, az_s.at[k], az_r.at[k], zfwd(k))

    def axc(k):
        s = win.at[zback_z(k), gh]
        return rcopy(s, s, ax_s.at[k], ax_r.at[k], xpeer)

    def axw(k):
        s = win.at[zback_z(k), 1 - gh]
        return rcopy(s, s, ax_s.at[k], ax_r.at[k], xpeer)

    bzc, bzw, byc, byw, bxc, bxw = gather(wo, bz_s, bz_r, by_s, by_r, bx_s, bx_r)

    lc_in[0].wait()
    lc_in[1].wait()
    loop(1, zs, lambda k: azc(k).start())

    e_up = rcopy(up_hbm.at[0], up.at[c], es.at[0], er.at[0], cpeer)
    e_down = rcopy(down_hbm.at[0], down.at[c], es.at[1], er.at[1], cpeer)
    e_up.start()
    e_down.start()
    lc_g.wait()

    def gcopy(d):
        return rcopy(gbuf.at[w], gbuf.at[w], gs.at[d], gr.at[d], {"wide": lax.rem(w + d, wide)})

    def gwait(d):
        s = gbuf.at[lax.rem(w + wide - d, wide)]
        return rcopy(s, s, gs.at[d], gr.at[d], {"wide": lax.rem(w + d, wide)})

    loop(1, wide, lambda d: gcopy(d).start())

    lc_tok.wait()
    step_rows = 32
    rin = nb.shape[4]

    def norm(i):
        rows = pl.ds(pl.multiple_of(i * step_rows, step_rows), step_rows)
        x = tok[rows, :].astype(F32)
        scale = lax.rsqrt(jnp.mean(x * x, axis=-1, keepdims=True) + 1e-05)
        n = (x * scale * gain_ref[...]).astype(BF16)
        part = i // (th // step_rows)
        within = pl.ds(pl.multiple_of(lax.rem(i, th // step_rows) * step_rows, step_rows), step_rows)
        for j in range(wide):
            nb[j % 2, part, j // 2, within, :] = n[:, j * rin : (j + 1) * rin]

    loop(0, tokens // step_rows, norm)

    tsend = rcopy(nb.at[oy, c], nby.at[c], ty_s, ty_r, ypeer)
    tsend.start()
    lc_out[0].wait()
    lc_out[1].wait()
    byc(0).start()

    def madd(zz):
        wb = win[zz].reshape(2 * half_in, lcols)
        for r in range(2):
            acc[r] += jnp.dot(nb[y, r, zz], wb, preferred_element_type=F32)
            acc[2 + r] += jnp.dot(nby[r, zz], wb, preferred_element_type=F32)

    acc[...] = jnp.zeros_like(acc)

    def z_arrive(k):
        azw(k).wait_recv()
        axc(k).start()

    loop(1, zs, z_arrive)
    loop(1, zs, lambda k: bzc(k).start())
    rcopy(nby.at[c], nby.at[c], ty_s, ty_r, ypeer).wait_recv()
    tfwd = rcopy(nby.at[c], nby.at[c], tc_s, tc_r, cpeer)
    tfwd.start()
    rcopy(nby.at[1 - c], nby.at[1 - c], tc_s, tc_r, cpeer).wait_recv()
    madd(z)

    def use_near(k):
        axw(k).wait_recv()
        madd(zback_z(k))

    loop(1, zs, use_near)
    psend[...] = acc[2:4].astype(BF16)
    pcopy = rcopy(psend, precv, py_s, py_r, ypeer)
    pcopy.start()
    bzw(1).wait_recv()
    bxc(1, False).start()
    byc(1).start()
    pcopy.wait_recv()

    lat[w, c] = (acc[c] + precv[c].astype(F32)).astype(BF16)
    xsend[...] = (acc[1 - c] + precv[1 - c].astype(F32)).astype(BF16)
    swap = rcopy(xsend, lat.at[w, c], cc_s, cc_r, cpeer)
    swap.start()
    rcopy(xsend, lat.at[w, 1 - c], cc_s, cc_r, cpeer).wait_recv()

    def czc(k):
        return rcopy(lat.at[w], lat.at[w], cz_s.at[k], cz_r.at[k], zfwd(k))

    def czw(k):
        s = lat.at[blk(k, y)]
        return rcopy(s, s, cz_s.at[k], cz_r.at[k], zfwd(k))

    def cyc(k):
        s = lat.at[blk(k, y)]
        return rcopy(s, s, cy_s.at[k], cy_r.at[k], ypeer)

    def cyw(k):
        s = lat.at[blk(k, oy)]
        return rcopy(s, s, cy_s.at[k], cy_r.at[k], ypeer)

    cyc(0).start()
    loop(1, zs, lambda k: czc(k).start())

    lc_up.wait()
    lc_down.wait()
    rcopy(up_hbm.at[0], up.at[1 - c], es.at[0], er.at[0], cpeer).wait_recv()
    rcopy(down_hbm.at[0], down.at[1 - c], es.at[1], er.at[1], cpeer).wait_recv()
    loop(1, wide, lambda d: gwait(d).wait_recv())

    def gate_col(b):
        gt = gbuf[b]
        mine = lax.broadcasted_iota(jnp.int32, gt.shape, 0) == w
        row = jnp.sum(jnp.where(mine, gt, 0.0), axis=0, keepdims=True)
        return jnp.transpose(jnp.broadcast_to(row, (8, th)))[:, :1]

    def dyc(k):
        return rcopy(ysend.at[k], yrecv.at[k], dy_s.at[k], dy_r.at[k], ypeer)

    def dzc(k):
        return rcopy(zsend.at[k], zrecv.at[k], dz_s.at[k], dz_r.at[k], zback(k))

    def expert(k):
        b0 = blk(k, 0)
        x0 = jnp.concatenate([lat[b0, 0], lat[b0 + 1, 0]], axis=0)
        x1 = jnp.concatenate([lat[b0, 1], lat[b0 + 1, 1]], axis=0)
        x = jnp.concatenate([x0, x1], axis=1)
        total = None
        for h in range(2):
            hid = lax.dot_general(x, up[h], (((1,), (1,)), ((), ())), preferred_element_type=F32)
            hid = jnp.square(jnp.maximum(hid, 0.0)).astype(BF16)
            part = jnp.dot(hid, down[h], preferred_element_type=F32)
            total = part if total is None else total + part
        obuf[0] = total[:th] * gate_col(b0)
        obuf[1] = total[th:] * gate_col(b0 + 1)
        ysend[k] = obuf[oy].astype(BF16)
        dyc(k).start()
        ownp[lax.rem(k, 2)] = obuf[y]

    def finish(k):
        dyc(k).wait_recv()
        zsend[k] = (ownp[lax.rem(k, 2)] + yrecv[k].astype(F32)).astype(BF16)
        dzc(k).start()

    def arrive(k):
        czw(k).wait_recv()
        cyc(k).start()

    loop(1, zs, arrive)
    cyw(0).wait_recv()
    expert(0)

    def b_arrive(k):
        bzw(k).wait_recv()
        bxc(k, False).start()

    loop(2, zs, b_arrive)

    def expert_step(k):
        cyw(k).wait_recv()
        expert(k)

        @pl.when(k > 1)
        def _():
            byc(k).start()
            finish(k - 1)

        @pl.when(k == 1)
        def _():
            dyc(0).wait_recv()
            macc[...] = ownp[0] + yrecv[0].astype(F32)

    loop(1, zs, expert_step)
    finish(zs - 1)

    def by_arrive(k):
        byw(k).wait_recv()
        bxc(k, True).start()

    loop(0, zs, by_arrive)

    def collect(k):
        dzc(k).wait_recv()
        macc[...] += zrecv[k].astype(F32)

    loop(1, zs, collect)
    mixb[c] = macc[...].astype(BF16)
    mcopy = rcopy(mixb.at[c], mixb.at[c], mc_s, mc_r, cpeer)
    mcopy.start()
    rcopy(mixb.at[1 - c], mixb.at[1 - c], mc_s, mc_r, cpeer).wait_recv()
    loop(1, zs, lambda k: bxw(k, False).wait_recv())
    loop(0, zs, lambda k: bxw(k, True).wait_recv())

    ocols = out_ref.shape[1]
    width = min(512, ocols)

    def project(i):
        m = mixb[...].reshape(tokens, mixb.shape[2])
        off = pl.multiple_of(i * width, width)
        wv = wo[:, :, :, pl.ds(off, width)].reshape(mixb.shape[2], width)
        branch = jnp.dot(m, wv, preferred_element_type=F32)
        own = tok[:, pl.ds(pl.multiple_of(c * ocols + off, width), width)].astype(F32)
        out_ref[:, pl.ds(off, width)] = (own + branch).astype(out_ref.dtype)

    loop(0, ocols // width, project)

    loop(1, wide, lambda d: gcopy(d).wait_send())
    e_up.wait_send()
    e_down.wait_send()
    swap.wait_send()
    mcopy.wait_send()
    tsend.wait_send()
    tfwd.wait_send()
    pcopy.wait_send()
    loop(1, zs, lambda k: azc(k).wait_send())
    loop(1, zs, lambda k: axc(k).wait_send())
    loop(1, zs, lambda k: bzc(k).wait_send())
    loop(0, zs, lambda k: byc(k).wait_send())
    loop(1, zs, lambda k: bxc(k, False).wait_send())
    loop(0, zs, lambda k: bxc(k, True).wait_send())
    loop(1, zs, lambda k: czc(k).wait_send())
    loop(0, zs, lambda k: cyc(k).wait_send())
    loop(0, zs, lambda k: dyc(k).wait_send())
    loop(1, zs, lambda k: dzc(k).wait_send())


def local(tokens, norm_gain, w_in, w_out, w_up, w_down, expert_ids, gate_weights):
    wide = lax.axis_size("wide")
    zs = wide // 2
    rows, depth = tokens.shape
    half = rows // 2
    latent = w_in.shape[1]
    ids = expert_ids.T
    chosen = ids[:, None, :] == jnp.arange(wide, dtype=jnp.int32)[None, :, None]
    gates = jnp.sum(jnp.where(chosen, gate_weights.T[:, None, :], 0.0), axis=0)
    gates = gates.reshape(wide, 2, half).transpose(1, 0, 2)
    any_ = pl.BlockSpec(memory_space=pl.ANY)
    vmem = pl.BlockSpec(memory_space=pltpu.VMEM)
    dma = pltpu.SemaphoreType.DMA
    hid = w_up.shape[2]
    cols = w_out.shape[1]
    V = pltpu.VMEM
    scratch = [
        V((rows, depth), BF16),
        V((2, 2, zs, half, depth // wide), BF16),
        V((2, zs, half, depth // wide), BF16),
        V((zs, 2, w_in.shape[0] // 2, latent // 2), BF16),
        V((wide, 2, w_out.shape[0] // 2, cols), BF16),
        V((2, hid, latent), BF16),
        V((2, hid, latent), BF16),
        V((wide, wide, half), F32),
        V((wide, 2, half, latent // 2), BF16),
        V((4, half, latent // 2), F32),
        V((2, half, latent // 2), BF16),
        V((2, half, latent // 2), BF16),
        V((half, latent // 2), BF16),
        V((2, half, latent), F32),
        V((2, half, latent), F32),
        V((zs, half, latent), BF16),
        V((zs, half, latent), BF16),
        V((zs, half, latent), BF16),
        V((zs, half, latent), BF16),
        V((half, latent), F32),
        V((2, half, latent), BF16),
        dma((8,)),
        dma((wide,)), dma((wide,)),
        dma((2,)), dma((2,)),
    ]
    scratch += [dma((zs,))] * 4 + [dma] * 6 + [dma((zs,))] * 4 + [dma((wide,))] * 2
    scratch += [dma((zs,))] * 4 + [dma, dma] + [dma((zs,))] * 4 + [dma, dma]
    return pl.pallas_call(
        kernel,
        out_shape=jax.ShapeDtypeStruct((rows, cols), BF16),
        in_specs=[any_, vmem, any_, any_, any_, any_, any_],
        out_specs=vmem,
        scratch_shapes=scratch,
        compiler_params=pltpu.CompilerParams(
            collective_id=0, has_side_effects=True, vmem_limit_bytes=66_000_000
        ),
        name="moe",
    )(tokens, norm_gain.reshape(1, depth), w_in, w_out, w_up.swapaxes(1, 2), w_down, gates)


def solution(mesh):
    in_specs = (
        P(("groups", "wide"), None),
        P(),
        P("wide", None),
        P("wide", "narrow"),
        P("wide", None, "narrow"),
        P("wide", "narrow", None),
        P(("groups", "wide"), None),
        P(("groups", "wide"), None),
    )
    out_specs = P(("groups", "wide"), "narrow")
    return jax.shard_map(local, mesh=mesh, in_specs=in_specs, out_specs=out_specs, check_vma=False)
```

```python
import functools
import jax
import jax.numpy as jnp
from jax import lax
from jax.experimental import pallas as pl
from jax.experimental.pallas import tpu as pltpu
from jax.sharding import PartitionSpec as P

F32 = jnp.float32
BF16 = jnp.bfloat16


def kernel(
    tok_hbm, gain_ref, win_hbm, wout_hbm, up_hbm, down_hbm, gates_hbm, out_ref,
    tok, nb, nby, win, wo, up, down, gbuf, lat, acc, psend, precv, xsend, obuf, ownp, ysend, yrecv, zsend, zrecv, macc, mixb,
    loc, gs, gr, es, er, az_s, az_r, ax_s, ax_r, ty_s, ty_r, tc_s, tc_r, py_s, py_r, bz_s, bz_r, by_s, by_r, bx_s, bx_r,
    cz_s, cz_r, cy_s, cy_r, cc_s, cc_r, dy_s, dy_r, dz_s, dz_r, mc_s, mc_r,
):
    wide = lax.axis_size("wide")
    zs = wide // 2
    g, w, c = lax.axis_index("groups"), lax.axis_index("wide"), lax.axis_index("narrow")
    z, y = w // 2, w % 2
    gh = g % 2
    xpeer = {"groups": g + 1 - 2 * gh}
    ypeer = {"wide": w + 1 - 2 * y}
    cpeer = {"narrow": 1 - c}
    MESH = pl.DeviceIdType.MESH

    def zfwd(k):
        return {"wide": lax.rem(z + k, zs) * 2 + y}

    def zback(k):
        return {"wide": lax.rem(z + zs - k, zs) * 2 + y}

    def blk(k, yy):
        return lax.rem(z + zs - k, zs) * 2 + yy

    def rcopy(src, dst, ss, rs, dev):
        return pltpu.make_async_remote_copy(
            src_ref=src, dst_ref=dst, send_sem=ss, recv_sem=rs, device_id=dev, device_id_type=MESH
        )

    def loop(lo, hi, body):
        def step(i, carry):
            body(i)
            return carry

        lax.fori_loop(lo, hi, step, 0)

    pieces, piece, lcols = win.shape[2:]
    half_out = wo.shape[2]
    tokens = tok.shape[0]
    th = lat.shape[2]
    oy = 1 - y

    in_cols = pl.ds(pl.multiple_of(c * lcols, lcols), lcols)
    lc_tok = pltpu.make_async_copy(tok_hbm, tok, loc.at[0])
    lc_in = [
        pltpu.make_async_copy(win_hbm.at[h, :, :, in_cols], win.at[z, h], loc.at[1 + h])
        for h in range(2)
    ]
    lc_out = [
        pltpu.make_async_copy(wout_hbm.at[pl.ds(h * half_out, half_out), :], wo.at[w, h], loc.at[3 + h])
        for h in range(2)
    ]
    lc_up = pltpu.make_async_copy(up_hbm.at[0], up.at[c], loc.at[5])
    lc_down = pltpu.make_async_copy(down_hbm.at[0], down.at[c], loc.at[6])
    lc_g = pltpu.make_async_copy(gates_hbm.at[c], gbuf.at[w], loc.at[7])
    for cp in lc_in + [lc_tok, lc_g, lc_up, lc_down] + lc_out:
        cp.start()

    barrier = pltpu.get_barrier_semaphore()
    loop(1, wide, lambda d: pl.semaphore_signal(
        barrier, inc=1, device_id={"wide": lax.rem(w + d, wide)}, device_id_type=MESH))
    pl.semaphore_signal(barrier, inc=1, device_id=xpeer, device_id_type=MESH)
    pl.semaphore_signal(barrier, inc=1, device_id=cpeer, device_id_type=MESH)
    pl.semaphore_wait(barrier, wide + 1)

    def gather(buf, z_s, z_r, y_s, y_r, x_s, x_r):
        def zc(k):
            return rcopy(buf.at[w, gh], buf.at[w, gh], z_s.at[k], z_r.at[k], zfwd(k))

        def zw(k):
            s = buf.at[blk(k, y), gh]
            return rcopy(s, s, z_s.at[k], z_r.at[k], zfwd(k))

        def yc(k):
            s = buf.at[blk(k, y), gh]
            return rcopy(s, s, y_s.at[k], y_r.at[k], ypeer)

        def yw(k):
            s = buf.at[blk(k, oy), gh]
            return rcopy(s, s, y_s.at[k], y_r.at[k], ypeer)

        def x_copy(k, far):
            s = buf.at[blk(k, oy if far else y), gh]
            i = k + zs if far else k
            return rcopy(s, s, x_s.at[i], x_r.at[i], xpeer)

        def x_wait(k, far):
            s = buf.at[blk(k, oy if far else y), 1 - gh]
            i = k + zs if far else k
            return rcopy(s, s, x_s.at[i], x_r.at[i], xpeer)

        return zc, zw, yc, yw, x_copy, x_wait

    def zback_z(k):
        return lax.rem(z + zs - k, zs)

    def azc(k, q):
        i = q * zs + k
        return rcopy(win.at[z, gh, q], win.at[z, gh, q], az_s.at[i], az_r.at[i], zfwd(k))

    def azw(k, q):
        s = win.at[zback_z(k), gh, q]
        i = q * zs + k
        return rcopy(s, s, az_s.at[i], az_r.at[i], zfwd(k))

    def axc(k, q):
        s = win.at[zback_z(k), gh, q]
        i = q * zs + k
        return rcopy(s, s, ax_s.at[i], ax_r.at[i], xpeer)

    def axw(k, q):
        s = win.at[zback_z(k), 1 - gh, q]
        i = q * zs + k
        return rcopy(s, s, ax_s.at[i], ax_r.at[i], xpeer)

    def each_piece(body):
        for q in range(pieces):
            loop(1, zs, lambda k: body(k, q))

    bzc, bzw, byc, byw, bxc, bxw = gather(wo, bz_s, bz_r, by_s, by_r, bx_s, bx_r)

    lc_in[0].wait()
    lc_in[1].wait()
    each_piece(lambda k, q: azc(k, q).start())

    e_up = rcopy(up_hbm.at[0], up.at[c], es.at[0], er.at[0], cpeer)
    e_down = rcopy(down_hbm.at[0], down.at[c], es.at[1], er.at[1], cpeer)
    e_up.start()
    e_down.start()
    lc_g.wait()

    def gcopy(d):
        return rcopy(gbuf.at[w], gbuf.at[w], gs.at[d], gr.at[d], {"wide": lax.rem(w + d, wide)})

    def gwait(d):
        s = gbuf.at[lax.rem(w + wide - d, wide)]
        return rcopy(s, s, gs.at[d], gr.at[d], {"wide": lax.rem(w + d, wide)})

    loop(1, wide, lambda d: gcopy(d).start())

    lc_tok.wait()
    step_rows = 32
    rin = nb.shape[4]

    def norm(i):
        rows = pl.ds(pl.multiple_of(i * step_rows, step_rows), step_rows)
        x = tok[rows, :].astype(F32)
        scale = lax.rsqrt(jnp.mean(x * x, axis=-1, keepdims=True) + 1e-05)
        n = (x * scale * gain_ref[...]).astype(BF16)
        part = i // (th // step_rows)
        within = pl.ds(pl.multiple_of(lax.rem(i, th // step_rows) * step_rows, step_rows), step_rows)
        for j in range(wide):
            nb[j % 2, part, j // 2, within, :] = n[:, j * rin : (j + 1) * rin]

    loop(0, tokens // step_rows, norm)

    tsend = rcopy(nb.at[oy, c], nby.at[c], ty_s, ty_r, ypeer)
    tsend.start()
    lc_out[0].wait()
    lc_out[1].wait()
    byc(0).start()

    def madd(zz):
        wb = win[zz].reshape(2 * pieces * piece, lcols)
        for r in range(2):
            acc[r] += jnp.dot(nb[y, r, zz], wb, preferred_element_type=F32)
            acc[2 + r] += jnp.dot(nby[r, zz], wb, preferred_element_type=F32)

    acc[...] = jnp.zeros_like(acc)

    def z_arrive(k, q):
        azw(k, q).wait_recv()
        axc(k, q).start()

    each_piece(z_arrive)
    loop(1, zs - 1, lambda k: bzc(k).start())
    rcopy(nby.at[c], nby.at[c], ty_s, ty_r, ypeer).wait_recv()
    tfwd = rcopy(nby.at[c], nby.at[c], tc_s, tc_r, cpeer)
    tfwd.start()
    rcopy(nby.at[1 - c], nby.at[1 - c], tc_s, tc_r, cpeer).wait_recv()
    madd(z)

    def use_near(k):
        for q in range(pieces):
            axw(k, q).wait_recv()
        madd(zback_z(k))

    loop(1, zs, use_near)
    psend[...] = acc[2:4].astype(BF16)
    pcopy = rcopy(psend, precv, py_s, py_r, ypeer)
    pcopy.start()
    bzw(1).wait_recv()
    bxc(1, False).start()
    byc(1).start()
    pcopy.wait_recv()

    hrow = th // 2

    def lpiece(b, q, r):
        return lat.at[b, q, pl.ds(r * hrow, hrow)]

    def czc(k, q, r):
        s = lpiece(w, q, r)
        i = (q * 2 + r) * zs + k
        return rcopy(s, s, cz_s.at[i], cz_r.at[i], zfwd(k))

    def czw(k, q, r):
        s = lpiece(blk(k, y), q, r)
        i = (q * 2 + r) * zs + k
        return rcopy(s, s, cz_s.at[i], cz_r.at[i], zfwd(k))

    def cyc(k, q, r):
        s = lpiece(blk(k, y), q, r)
        i = (q * 2 + r) * zs + k
        return rcopy(s, s, cy_s.at[i], cy_r.at[i], ypeer)

    def cyw(k, q, r):
        s = lpiece(blk(k, oy), q, r)
        i = (q * 2 + r) * zs + k
        return rcopy(s, s, cy_s.at[i], cy_r.at[i], ypeer)

    xsend[...] = (acc[1 - c] + precv[1 - c].astype(F32)).astype(BF16)
    swap = rcopy(xsend, lat.at[w, c], cc_s, cc_r, cpeer)
    swap.start()
    lat[w, c] = (acc[c] + precv[c].astype(F32)).astype(BF16)
    for r in range(2):
        cyc(0, c, r).start()
        loop(1, zs, lambda k: czc(k, c, r).start())
    rcopy(xsend, lat.at[w, 1 - c], cc_s, cc_r, cpeer).wait_recv()
    for r in range(2):
        cyc(0, 1 - c, r).start()
        loop(1, zs, lambda k: czc(k, 1 - c, r).start())
    loop(zs - 1, zs, lambda k: bzc(k).start())

    lc_up.wait()
    lc_down.wait()
    rcopy(up_hbm.at[0], up.at[1 - c], es.at[0], er.at[0], cpeer).wait_recv()
    rcopy(down_hbm.at[0], down.at[1 - c], es.at[1], er.at[1], cpeer).wait_recv()
    loop(1, wide, lambda d: gwait(d).wait_recv())

    def gate_col(b):
        gt = gbuf[b]
        mine = lax.broadcasted_iota(jnp.int32, gt.shape, 0) == w
        row = jnp.sum(jnp.where(mine, gt, 0.0), axis=0, keepdims=True)
        return jnp.transpose(jnp.broadcast_to(row, (8, th)))[:, :1]

    def dyc(k):
        return rcopy(ysend.at[k], yrecv.at[k], dy_s.at[k], dy_r.at[k], ypeer)

    def dzc(k):
        return rcopy(zsend.at[k], zrecv.at[k], dz_s.at[k], dz_r.at[k], zback(k))

    def expert(k):
        b0 = blk(k, 0)
        x0 = jnp.concatenate([lat[b0, 0], lat[b0 + 1, 0]], axis=0)
        x1 = jnp.concatenate([lat[b0, 1], lat[b0 + 1, 1]], axis=0)
        x = jnp.concatenate([x0, x1], axis=1)
        total = None
        for h in range(2):
            hid = lax.dot_general(x, up[h], (((1,), (1,)), ((), ())), preferred_element_type=F32)
            hid = jnp.square(jnp.maximum(hid, 0.0)).astype(BF16)
            part = jnp.dot(hid, down[h], preferred_element_type=F32)
            total = part if total is None else total + part
        obuf[0] = total[:th] * gate_col(b0)
        obuf[1] = total[th:] * gate_col(b0 + 1)
        ysend[k] = obuf[oy].astype(BF16)
        dyc(k).start()
        ownp[lax.rem(k, 2)] = obuf[y]

    def finish(k):
        dyc(k).wait_recv()
        zsend[k] = (ownp[lax.rem(k, 2)] + yrecv[k].astype(F32)).astype(BF16)
        dzc(k).start()

    order = [(q, r) for q in (c, 1 - c) for r in range(2)]

    def arrive(k, q, r):
        czw(k, q, r).wait_recv()
        cyc(k, q, r).start()

    for q, r in order:
        loop(1, zs, lambda k: arrive(k, q, r))

    def far_rows(k):
        for q, r in order:
            cyw(k, q, r).wait_recv()

    far_rows(0)
    expert(0)

    def b_arrive(k):
        bzw(k).wait_recv()
        bxc(k, False).start()

    loop(2, zs, b_arrive)

    def expert_step(k):
        far_rows(k)
        expert(k)

        @pl.when(k > 1)
        def _():
            byc(k).start()
            finish(k - 1)

        @pl.when(k == 1)
        def _():
            dyc(0).wait_recv()
            macc[...] = ownp[0] + yrecv[0].astype(F32)

    loop(1, zs, expert_step)
    finish(zs - 1)

    def by_arrive(k):
        byw(k).wait_recv()
        bxc(k, True).start()

    loop(0, zs, by_arrive)

    def collect(k):
        dzc(k).wait_recv()
        macc[...] += zrecv[k].astype(F32)

    loop(1, zs, collect)
    mixb[c] = macc[...].astype(BF16)
    mcopy = rcopy(mixb.at[c], mixb.at[c], mc_s, mc_r, cpeer)
    mcopy.start()
    rcopy(mixb.at[1 - c], mixb.at[1 - c], mc_s, mc_r, cpeer).wait_recv()
    loop(1, zs, lambda k: bxw(k, False).wait_recv())
    loop(0, zs, lambda k: bxw(k, True).wait_recv())

    ocols = out_ref.shape[1]
    width = min(512, ocols)

    def project(i):
        m = mixb[...].reshape(tokens, mixb.shape[2])
        off = pl.multiple_of(i * width, width)
        wv = wo[:, :, :, pl.ds(off, width)].reshape(mixb.shape[2], width)
        branch = jnp.dot(m, wv, preferred_element_type=F32)
        own = tok[:, pl.ds(pl.multiple_of(c * ocols + off, width), width)].astype(F32)
        out_ref[:, pl.ds(off, width)] = (own + branch).astype(out_ref.dtype)

    loop(0, ocols // width, project)

    loop(1, wide, lambda d: gcopy(d).wait_send())
    e_up.wait_send()
    e_down.wait_send()
    swap.wait_send()
    mcopy.wait_send()
    tsend.wait_send()
    tfwd.wait_send()
    pcopy.wait_send()
    each_piece(lambda k, q: azc(k, q).wait_send())
    each_piece(lambda k, q: axc(k, q).wait_send())
    loop(1, zs, lambda k: bzc(k).wait_send())
    loop(0, zs, lambda k: byc(k).wait_send())
    loop(1, zs, lambda k: bxc(k, False).wait_send())
    loop(0, zs, lambda k: bxc(k, True).wait_send())
    for q, r in order:
        loop(1, zs, lambda k: czc(k, q, r).wait_send())
        loop(0, zs, lambda k: cyc(k, q, r).wait_send())
    loop(0, zs, lambda k: dyc(k).wait_send())
    loop(1, zs, lambda k: dzc(k).wait_send())


def local(tokens, norm_gain, w_in, w_out, w_up, w_down, expert_ids, gate_weights):
    wide = lax.axis_size("wide")
    zs = wide // 2
    rows, depth = tokens.shape
    half = rows // 2
    latent = w_in.shape[1]
    pieces = 4
    piece = w_in.shape[0] // (2 * pieces)
    ids = expert_ids.T
    chosen = ids[:, None, :] == jnp.arange(wide, dtype=jnp.int32)[None, :, None]
    gates = jnp.sum(jnp.where(chosen, gate_weights.T[:, None, :], 0.0), axis=0)
    gates = gates.reshape(wide, 2, half).transpose(1, 0, 2)
    any_ = pl.BlockSpec(memory_space=pl.ANY)
    vmem = pl.BlockSpec(memory_space=pltpu.VMEM)
    dma = pltpu.SemaphoreType.DMA
    hid = w_up.shape[2]
    cols = w_out.shape[1]
    V = pltpu.VMEM
    scratch = [
        V((rows, depth), BF16),
        V((2, 2, zs, half, depth // wide), BF16),
        V((2, zs, half, depth // wide), BF16),
        V((zs, 2, pieces, piece, latent // 2), BF16),
        V((wide, 2, w_out.shape[0] // 2, cols), BF16),
        V((2, hid, latent), BF16),
        V((2, hid, latent), BF16),
        V((wide, wide, half), F32),
        V((wide, 2, half, latent // 2), BF16),
        V((4, half, latent // 2), F32),
        V((2, half, latent // 2), BF16),
        V((2, half, latent // 2), BF16),
        V((half, latent // 2), BF16),
        V((2, half, latent), F32),
        V((2, half, latent), F32),
        V((zs, half, latent), BF16),
        V((zs, half, latent), BF16),
        V((zs, half, latent), BF16),
        V((zs, half, latent), BF16),
        V((half, latent), F32),
        V((2, half, latent), BF16),
        dma((8,)),
        dma((wide,)), dma((wide,)),
        dma((2,)), dma((2,)),
    ]
    scratch += [dma((pieces * zs,))] * 4 + [dma] * 6 + [dma((zs,))] * 4 + [dma((wide,))] * 2
    scratch += [dma((4 * zs,))] * 4 + [dma, dma] + [dma((zs,))] * 4 + [dma, dma]
    return pl.pallas_call(
        kernel,
        out_shape=jax.ShapeDtypeStruct((rows, cols), BF16),
        in_specs=[any_, vmem, any_, any_, any_, any_, any_],
        out_specs=vmem,
        scratch_shapes=scratch,
        compiler_params=pltpu.CompilerParams(
            collective_id=0, has_side_effects=True, vmem_limit_bytes=66_000_000
        ),
        name="moe",
    )(tokens, norm_gain.reshape(1, depth), w_in.reshape(2, pieces, piece, latent), w_out, w_up.swapaxes(1, 2), w_down, gates)


def solution(mesh):
    in_specs = (
        P(("groups", "wide"), None),
        P(),
        P("wide", None),
        P("wide", "narrow"),
        P("wide", None, "narrow"),
        P("wide", "narrow", None),
        P(("groups", "wide"), None),
        P(("groups", "wide"), None),
    )
    out_specs = P(("groups", "wide"), "narrow")
    return jax.shard_map(local, mesh=mesh, in_specs=in_specs, out_specs=out_specs, check_vma=False)
```

```python
import functools
import jax
import jax.numpy as jnp
from jax import lax
from jax.experimental import pallas as pl
from jax.experimental.pallas import tpu as pltpu
from jax.sharding import PartitionSpec as P

F32 = jnp.float32
BF16 = jnp.bfloat16


def kernel(
    tok_hbm, gain_ref, win_hbm, wout_hbm, up_hbm, down_hbm, gates_hbm, out_ref,
    tok, nb, nby, win, wo, up, down, gbuf, lat, acc, psend, precv, xsend, obuf, ownp, ysend, yrecv, zsend, zrecv, macc, mixb,
    loc, gs, gr, es, er, az_s, az_r, ax_s, ax_r, ty_s, ty_r, tc_s, tc_r, py_s, py_r, bz_s, bz_r, by_s, by_r, bx_s, bx_r,
    cz_s, cz_r, cy_s, cy_r, cc_s, cc_r, dy_s, dy_r, dz_s, dz_r, mc_s, mc_r,
):
    wide = lax.axis_size("wide")
    zs = wide // 2
    g, w, c = lax.axis_index("groups"), lax.axis_index("wide"), lax.axis_index("narrow")
    z, y = w // 2, w % 2
    gh = g % 2
    xpeer = {"groups": g + 1 - 2 * gh}
    ypeer = {"wide": w + 1 - 2 * y}
    cpeer = {"narrow": 1 - c}
    MESH = pl.DeviceIdType.MESH

    def zfwd(k):
        return {"wide": lax.rem(z + k, zs) * 2 + y}

    def zback(k):
        return {"wide": lax.rem(z + zs - k, zs) * 2 + y}

    def blk(k, yy):
        return lax.rem(z + zs - k, zs) * 2 + yy

    def rcopy(src, dst, ss, rs, dev):
        return pltpu.make_async_remote_copy(
            src_ref=src, dst_ref=dst, send_sem=ss, recv_sem=rs, device_id=dev, device_id_type=MESH
        )

    def loop(lo, hi, body):
        def step(i, carry):
            body(i)
            return carry

        lax.fori_loop(lo, hi, step, 0)

    pieces, piece, lcols = win.shape[2:]
    half_out = wo.shape[2]
    tokens = tok.shape[0]
    th = lat.shape[2]
    oy = 1 - y

    in_cols = pl.ds(pl.multiple_of(c * lcols, lcols), lcols)
    lc_tok = pltpu.make_async_copy(tok_hbm, tok, loc.at[0])
    lc_in = [
        pltpu.make_async_copy(win_hbm.at[h, :, :, in_cols], win.at[z, h], loc.at[1 + h])
        for h in range(2)
    ]
    lc_out = [
        pltpu.make_async_copy(wout_hbm.at[pl.ds(h * half_out, half_out), :], wo.at[w, h], loc.at[3 + h])
        for h in range(2)
    ]
    lc_up = pltpu.make_async_copy(up_hbm.at[0], up.at[c], loc.at[5])
    lc_down = pltpu.make_async_copy(down_hbm.at[0], down.at[c], loc.at[6])
    lc_g = pltpu.make_async_copy(gates_hbm.at[c], gbuf.at[w], loc.at[7])
    for cp in lc_in + [lc_tok, lc_g, lc_up, lc_down] + lc_out:
        cp.start()

    barrier = pltpu.get_barrier_semaphore()
    loop(1, wide, lambda d: pl.semaphore_signal(
        barrier, inc=1, device_id={"wide": lax.rem(w + d, wide)}, device_id_type=MESH))
    pl.semaphore_signal(barrier, inc=1, device_id=xpeer, device_id_type=MESH)
    pl.semaphore_signal(barrier, inc=1, device_id=cpeer, device_id_type=MESH)
    pl.semaphore_wait(barrier, wide + 1)

    def gather(buf, z_s, z_r, y_s, y_r, x_s, x_r):
        def zc(k):
            return rcopy(buf.at[w, gh], buf.at[w, gh], z_s.at[k], z_r.at[k], zfwd(k))

        def zw(k):
            s = buf.at[blk(k, y), gh]
            return rcopy(s, s, z_s.at[k], z_r.at[k], zfwd(k))

        def yc(k):
            s = buf.at[blk(k, y), gh]
            return rcopy(s, s, y_s.at[k], y_r.at[k], ypeer)

        def yw(k):
            s = buf.at[blk(k, oy), gh]
            return rcopy(s, s, y_s.at[k], y_r.at[k], ypeer)

        def x_copy(k, far):
            s = buf.at[blk(k, oy if far else y), gh]
            i = k + zs if far else k
            return rcopy(s, s, x_s.at[i], x_r.at[i], xpeer)

        def x_wait(k, far):
            s = buf.at[blk(k, oy if far else y), 1 - gh]
            i = k + zs if far else k
            return rcopy(s, s, x_s.at[i], x_r.at[i], xpeer)

        return zc, zw, yc, yw, x_copy, x_wait

    def zback_z(k):
        return lax.rem(z + zs - k, zs)

    def azc(k, q):
        i = q * zs + k
        return rcopy(win.at[z, gh, q], win.at[z, gh, q], az_s.at[i], az_r.at[i], zfwd(k))

    def azw(k, q):
        s = win.at[zback_z(k), gh, q]
        i = q * zs + k
        return rcopy(s, s, az_s.at[i], az_r.at[i], zfwd(k))

    def axc(k, q):
        s = win.at[zback_z(k), gh, q]
        i = q * zs + k
        return rcopy(s, s, ax_s.at[i], ax_r.at[i], xpeer)

    def axw(k, q):
        s = win.at[zback_z(k), 1 - gh, q]
        i = q * zs + k
        return rcopy(s, s, ax_s.at[i], ax_r.at[i], xpeer)

    def each_piece(body):
        for q in range(pieces):
            loop(1, zs, lambda k: body(k, q))

    bzc, bzw, byc, byw, bxc, bxw = gather(wo, bz_s, bz_r, by_s, by_r, bx_s, bx_r)

    lc_in[0].wait()
    lc_in[1].wait()
    each_piece(lambda k, q: azc(k, q).start())

    e_up = rcopy(up_hbm.at[0], up.at[c], es.at[0], er.at[0], cpeer)
    e_down = rcopy(down_hbm.at[0], down.at[c], es.at[1], er.at[1], cpeer)
    e_up.start()
    e_down.start()
    lc_g.wait()

    def gcopy(d):
        return rcopy(gbuf.at[w], gbuf.at[w], gs.at[d], gr.at[d], {"wide": lax.rem(w + d, wide)})

    def gwait(d):
        s = gbuf.at[lax.rem(w + wide - d, wide)]
        return rcopy(s, s, gs.at[d], gr.at[d], {"wide": lax.rem(w + d, wide)})

    loop(1, wide, lambda d: gcopy(d).start())

    lc_tok.wait()
    step_rows = 32
    rin = nb.shape[4]

    def norm(i):
        rows = pl.ds(pl.multiple_of(i * step_rows, step_rows), step_rows)
        x = tok[rows, :].astype(F32)
        scale = lax.rsqrt(jnp.mean(x * x, axis=-1, keepdims=True) + 1e-05)
        n = (x * scale * gain_ref[...]).astype(BF16)
        part = i // (th // step_rows)
        within = pl.ds(pl.multiple_of(lax.rem(i, th // step_rows) * step_rows, step_rows), step_rows)
        for j in range(wide):
            nb[j % 2, part, j // 2, within, :] = n[:, j * rin : (j + 1) * rin]

    loop(0, tokens // step_rows, norm)

    tsend = rcopy(nb.at[oy, c], nby.at[c], ty_s, ty_r, ypeer)
    tsend.start()
    lc_out[0].wait()
    lc_out[1].wait()
    byc(0).start()

    def madd(zz):
        wb = win[zz].reshape(2 * pieces * piece, lcols)
        for r in range(2):
            acc[r] += jnp.dot(nb[y, r, zz], wb, preferred_element_type=F32)
            acc[2 + r] += jnp.dot(nby[r, zz], wb, preferred_element_type=F32)

    acc[...] = jnp.zeros_like(acc)

    def z_arrive(k, q):
        azw(k, q).wait_recv()
        axc(k, q).start()

    each_piece(z_arrive)
    loop(1, zs - 1, lambda k: bzc(k).start())
    rcopy(nby.at[c], nby.at[c], ty_s, ty_r, ypeer).wait_recv()
    tfwd = rcopy(nby.at[c], nby.at[c], tc_s, tc_r, cpeer)
    tfwd.start()
    rcopy(nby.at[1 - c], nby.at[1 - c], tc_s, tc_r, cpeer).wait_recv()
    madd(z)

    def use_near(k):
        for q in range(pieces):
            axw(k, q).wait_recv()
        madd(zback_z(k))

    loop(1, zs, use_near)
    psend[...] = acc[2:4].astype(BF16)
    pcopy = rcopy(psend, precv, py_s, py_r, ypeer)
    pcopy.start()
    bzw(1).wait_recv()
    bxc(1, False).start()
    byc(1).start()
    pcopy.wait_recv()

    hrow = th // 2

    def lpiece(b, q, r):
        return lat.at[b, q, pl.ds(r * hrow, hrow)]

    def czc(k, q, r):
        s = lpiece(w, q, r)
        i = (q * 2 + r) * zs + k
        return rcopy(s, s, cz_s.at[i], cz_r.at[i], zfwd(k))

    def czw(k, q, r):
        s = lpiece(blk(k, y), q, r)
        i = (q * 2 + r) * zs + k
        return rcopy(s, s, cz_s.at[i], cz_r.at[i], zfwd(k))

    def cyc(k, q, r):
        s = lpiece(blk(k, y), q, r)
        i = (q * 2 + r) * zs + k
        return rcopy(s, s, cy_s.at[i], cy_r.at[i], ypeer)

    def cyw(k, q, r):
        s = lpiece(blk(k, oy), q, r)
        i = (q * 2 + r) * zs + k
        return rcopy(s, s, cy_s.at[i], cy_r.at[i], ypeer)

    xsend[...] = (acc[1 - c] + precv[1 - c].astype(F32)).astype(BF16)
    swap = rcopy(xsend, lat.at[w, c], cc_s, cc_r, cpeer)
    swap.start()
    lat[w, c] = (acc[c] + precv[c].astype(F32)).astype(BF16)
    for r in range(2):
        cyc(0, c, r).start()
        czc(1, c, r).start()
    rcopy(xsend, lat.at[w, 1 - c], cc_s, cc_r, cpeer).wait_recv()
    for r in range(2):
        cyc(0, 1 - c, r).start()
        czc(1, 1 - c, r).start()

    def later(k):
        for q in (c, 1 - c):
            for r in range(2):
                czc(k, q, r).start()

    loop(2, zs, later)
    loop(zs - 1, zs, lambda k: bzc(k).start())

    lc_up.wait()
    lc_down.wait()
    rcopy(up_hbm.at[0], up.at[1 - c], es.at[0], er.at[0], cpeer).wait_recv()
    rcopy(down_hbm.at[0], down.at[1 - c], es.at[1], er.at[1], cpeer).wait_recv()
    loop(1, wide, lambda d: gwait(d).wait_recv())

    def gate_col(b):
        gt = gbuf[b]
        mine = lax.broadcasted_iota(jnp.int32, gt.shape, 0) == w
        row = jnp.sum(jnp.where(mine, gt, 0.0), axis=0, keepdims=True)
        return jnp.transpose(jnp.broadcast_to(row, (8, th)))[:, :1]

    hcol = ysend.shape[3]

    def dyc(k, q):
        i = q * zs + k
        return rcopy(ysend.at[k, q], yrecv.at[k, q], dy_s.at[i], dy_r.at[i], ypeer)

    def dzc(k, q):
        i = q * zs + k
        return rcopy(zsend.at[k, q], zrecv.at[k, q], dz_s.at[i], dz_r.at[i], zback(k))

    def expert(k):
        b0 = blk(k, 0)
        x0 = jnp.concatenate([lat[b0, 0], lat[b0 + 1, 0]], axis=0)
        x1 = jnp.concatenate([lat[b0, 1], lat[b0 + 1, 1]], axis=0)
        x = jnp.concatenate([x0, x1], axis=1)
        total = None
        for h in range(2):
            hid = lax.dot_general(x, up[h], (((1,), (1,)), ((), ())), preferred_element_type=F32)
            hid = jnp.square(jnp.maximum(hid, 0.0)).astype(BF16)
            part = jnp.dot(hid, down[h], preferred_element_type=F32)
            total = part if total is None else total + part
        obuf[0] = total[:th] * gate_col(b0)
        obuf[1] = total[th:] * gate_col(b0 + 1)
        for q in range(2):
            ysend[k, q] = obuf[oy, :, q * hcol : (q + 1) * hcol].astype(BF16)
            dyc(k, q).start()
        ownp[lax.rem(k, 2)] = obuf[y]

    def finish(k):
        for q in range(2):
            dyc(k, q).wait_recv()
            own = ownp[lax.rem(k, 2), :, q * hcol : (q + 1) * hcol]
            zsend[k, q] = (own + yrecv[k, q].astype(F32)).astype(BF16)
            dzc(k, q).start()

    order = [(q, r) for q in (c, 1 - c) for r in range(2)]

    def arrive(k, q, r):
        czw(k, q, r).wait_recv()
        cyc(k, q, r).start()

    def arrive_all(k):
        for q, r in order:
            arrive(k, q, r)

    def far_rows(k):
        for q, r in order:
            cyw(k, q, r).wait_recv()

    def b_arrive(k):
        bzw(k).wait_recv()
        bxc(k, False).start()
        byc(k).start()

    def by_arrive(k):
        byw(k).wait_recv()
        bxc(k, True).start()

    arrive_all(1)
    far_rows(0)
    expert(0)
    by_arrive(0)

    def expert_step(k):
        @pl.when(k < zs - 1)
        def _():
            arrive_all(k + 1)

        far_rows(k)
        expert(k)

        @pl.when(k > 1)
        def _():
            finish(k - 1)

        @pl.when(k == 1)
        def _():
            for q in range(2):
                dyc(0, q).wait_recv()
                cols = slice(q * hcol, (q + 1) * hcol)
                macc[:, cols] = ownp[0, :, cols] + yrecv[0, q].astype(F32)
            by_arrive(1)

        @pl.when((k > 1) & (k < zs - 1))
        def _():
            b_arrive(k)

    loop(1, zs, expert_step)
    loop(zs - 1, zs, b_arrive)
    finish(zs - 1)
    loop(2, zs, by_arrive)

    def collect(k):
        for q in range(2):
            dzc(k, q).wait_recv()
            macc[:, q * hcol : (q + 1) * hcol] += zrecv[k, q].astype(F32)

    loop(1, zs, collect)
    mixb[c] = macc[...].astype(BF16)
    mcopy = rcopy(mixb.at[c], mixb.at[c], mc_s, mc_r, cpeer)
    mcopy.start()
    rcopy(mixb.at[1 - c], mixb.at[1 - c], mc_s, mc_r, cpeer).wait_recv()
    loop(1, zs, lambda k: bxw(k, False).wait_recv())
    loop(0, zs, lambda k: bxw(k, True).wait_recv())

    ocols = out_ref.shape[1]
    width = min(512, ocols)

    def project(i):
        m = mixb[...].reshape(tokens, mixb.shape[2])
        off = pl.multiple_of(i * width, width)
        wv = wo[:, :, :, pl.ds(off, width)].reshape(mixb.shape[2], width)
        branch = jnp.dot(m, wv, preferred_element_type=F32)
        own = tok[:, pl.ds(pl.multiple_of(c * ocols + off, width), width)].astype(F32)
        out_ref[:, pl.ds(off, width)] = (own + branch).astype(out_ref.dtype)

    loop(0, ocols // width, project)

    loop(1, wide, lambda d: gcopy(d).wait_send())
    e_up.wait_send()
    e_down.wait_send()
    swap.wait_send()
    mcopy.wait_send()
    tsend.wait_send()
    tfwd.wait_send()
    pcopy.wait_send()
    each_piece(lambda k, q: azc(k, q).wait_send())
    each_piece(lambda k, q: axc(k, q).wait_send())
    loop(1, zs, lambda k: bzc(k).wait_send())
    loop(0, zs, lambda k: byc(k).wait_send())
    loop(1, zs, lambda k: bxc(k, False).wait_send())
    loop(0, zs, lambda k: bxc(k, True).wait_send())
    for q, r in order:
        loop(1, zs, lambda k: czc(k, q, r).wait_send())
        loop(0, zs, lambda k: cyc(k, q, r).wait_send())
    for q in range(2):
        loop(0, zs, lambda k: dyc(k, q).wait_send())
        loop(1, zs, lambda k: dzc(k, q).wait_send())


def local(tokens, norm_gain, w_in, w_out, w_up, w_down, expert_ids, gate_weights):
    wide = lax.axis_size("wide")
    zs = wide // 2
    rows, depth = tokens.shape
    half = rows // 2
    latent = w_in.shape[1]
    pieces = 4
    piece = w_in.shape[0] // (2 * pieces)
    ids = expert_ids.T
    chosen = ids[:, None, :] == jnp.arange(wide, dtype=jnp.int32)[None, :, None]
    gates = jnp.sum(jnp.where(chosen, gate_weights.T[:, None, :], 0.0), axis=0)
    gates = gates.reshape(wide, 2, half).transpose(1, 0, 2)
    any_ = pl.BlockSpec(memory_space=pl.ANY)
    vmem = pl.BlockSpec(memory_space=pltpu.VMEM)
    dma = pltpu.SemaphoreType.DMA
    hid = w_up.shape[2]
    cols = w_out.shape[1]
    V = pltpu.VMEM
    scratch = [
        V((rows, depth), BF16),
        V((2, 2, zs, half, depth // wide), BF16),
        V((2, zs, half, depth // wide), BF16),
        V((zs, 2, pieces, piece, latent // 2), BF16),
        V((wide, 2, w_out.shape[0] // 2, cols), BF16),
        V((2, hid, latent), BF16),
        V((2, hid, latent), BF16),
        V((wide, wide, half), F32),
        V((wide, 2, half, latent // 2), BF16),
        V((4, half, latent // 2), F32),
        V((2, half, latent // 2), BF16),
        V((2, half, latent // 2), BF16),
        V((half, latent // 2), BF16),
        V((2, half, latent), F32),
        V((2, half, latent), F32),
        V((zs, 2, half, latent // 2), BF16),
        V((zs, 2, half, latent // 2), BF16),
        V((zs, 2, half, latent // 2), BF16),
        V((zs, 2, half, latent // 2), BF16),
        V((half, latent), F32),
        V((2, half, latent), BF16),
        dma((8,)),
        dma((wide,)), dma((wide,)),
        dma((2,)), dma((2,)),
    ]
    scratch += [dma((pieces * zs,))] * 4 + [dma] * 6 + [dma((zs,))] * 4 + [dma((wide,))] * 2
    scratch += [dma((4 * zs,))] * 4 + [dma, dma] + [dma((2 * zs,))] * 4 + [dma, dma]
    return pl.pallas_call(
        kernel,
        out_shape=jax.ShapeDtypeStruct((rows, cols), BF16),
        in_specs=[any_, vmem, any_, any_, any_, any_, any_],
        out_specs=vmem,
        scratch_shapes=scratch,
        compiler_params=pltpu.CompilerParams(
            collective_id=0, has_side_effects=True, vmem_limit_bytes=66_000_000
        ),
        name="moe",
    )(tokens, norm_gain.reshape(1, depth), w_in.reshape(2, pieces, piece, latent), w_out, w_up.swapaxes(1, 2), w_down, gates)


def solution(mesh):
    in_specs = (
        P(("groups", "wide"), None),
        P(),
        P("wide", None),
        P("wide", "narrow"),
        P("wide", None, "narrow"),
        P("wide", "narrow", None),
        P(("groups", "wide"), None),
        P(("groups", "wide"), None),
    )
    out_specs = P(("groups", "wide"), "narrow")
    return jax.shard_map(local, mesh=mesh, in_specs=in_specs, out_specs=out_specs, check_vma=False)
```

```python
import functools
import jax
import jax.numpy as jnp
from jax import lax
from jax.experimental import pallas as pl
from jax.experimental.pallas import tpu as pltpu
from jax.sharding import PartitionSpec as P

F32 = jnp.float32
BF16 = jnp.bfloat16


def kernel(
    tok_hbm, gain_ref, win_hbm, wout_hbm, up_hbm, down_hbm, gates_hbm, out_ref,
    tok, nb, nby, win, wo, up, down, gbuf, lat, acc, psend, precv, xsend, obuf, ownp, ysend, yrecv, zsend, zrecv, macc, mixb,
    loc, gs, gr, es, er, az_s, az_r, ax_s, ax_r, ty_s, ty_r, tc_s, tc_r, py_s, py_r, bz_s, bz_r, by_s, by_r, bx_s, bx_r,
    cz_s, cz_r, cy_s, cy_r, cc_s, cc_r, dy_s, dy_r, dz_s, dz_r, mc_s, mc_r,
):
    wide = lax.axis_size("wide")
    zs = wide // 2
    g, w, c = lax.axis_index("groups"), lax.axis_index("wide"), lax.axis_index("narrow")
    z, y = w // 2, w % 2
    gh = g % 2
    xpeer = {"groups": g + 1 - 2 * gh}
    ypeer = {"wide": w + 1 - 2 * y}
    cpeer = {"narrow": 1 - c}
    MESH = pl.DeviceIdType.MESH

    def zfwd(k):
        return {"wide": lax.rem(z + k, zs) * 2 + y}

    def zback(k):
        return {"wide": lax.rem(z + zs - k, zs) * 2 + y}

    def blk(k, yy):
        return lax.rem(z + zs - k, zs) * 2 + yy

    def rcopy(src, dst, ss, rs, dev):
        return pltpu.make_async_remote_copy(
            src_ref=src, dst_ref=dst, send_sem=ss, recv_sem=rs, device_id=dev, device_id_type=MESH
        )

    def loop(lo, hi, body):
        def step(i, carry):
            body(i)
            return carry

        lax.fori_loop(lo, hi, step, 0)

    pieces, piece, lcols = win.shape[2:]
    half_out = wo.shape[2]
    tokens = tok.shape[0]
    th = lat.shape[2]
    oy = 1 - y

    in_cols = pl.ds(pl.multiple_of(c * lcols, lcols), lcols)
    lc_tok = pltpu.make_async_copy(tok_hbm, tok, loc.at[0])
    lc_in = [
        pltpu.make_async_copy(win_hbm.at[h, :, :, in_cols], win.at[z, h], loc.at[1 + h])
        for h in range(2)
    ]
    lc_out = [
        pltpu.make_async_copy(wout_hbm.at[pl.ds(h * half_out, half_out), :], wo.at[w, h], loc.at[3 + h])
        for h in range(2)
    ]
    lc_up = pltpu.make_async_copy(up_hbm.at[0], up.at[c], loc.at[5])
    lc_down = pltpu.make_async_copy(down_hbm.at[0], down.at[c], loc.at[6])
    lc_g = pltpu.make_async_copy(gates_hbm.at[c], gbuf.at[w], loc.at[7])
    for cp in lc_in + [lc_tok, lc_g, lc_up, lc_down] + lc_out:
        cp.start()

    barrier = pltpu.get_barrier_semaphore()
    loop(1, wide, lambda d: pl.semaphore_signal(
        barrier, inc=1, device_id={"wide": lax.rem(w + d, wide)}, device_id_type=MESH))
    pl.semaphore_signal(barrier, inc=1, device_id=xpeer, device_id_type=MESH)
    pl.semaphore_signal(barrier, inc=1, device_id=cpeer, device_id_type=MESH)
    pl.semaphore_wait(barrier, wide + 1)

    def gather(buf, z_s, z_r, y_s, y_r, x_s, x_r):
        def zc(k):
            return rcopy(buf.at[w, gh], buf.at[w, gh], z_s.at[k], z_r.at[k], zfwd(k))

        def zw(k):
            s = buf.at[blk(k, y), gh]
            return rcopy(s, s, z_s.at[k], z_r.at[k], zfwd(k))

        def yc(k):
            s = buf.at[blk(k, y), gh]
            return rcopy(s, s, y_s.at[k], y_r.at[k], ypeer)

        def yw(k):
            s = buf.at[blk(k, oy), gh]
            return rcopy(s, s, y_s.at[k], y_r.at[k], ypeer)

        def x_copy(k, far):
            s = buf.at[blk(k, oy if far else y), gh]
            i = k + zs if far else k
            return rcopy(s, s, x_s.at[i], x_r.at[i], xpeer)

        def x_wait(k, far):
            s = buf.at[blk(k, oy if far else y), 1 - gh]
            i = k + zs if far else k
            return rcopy(s, s, x_s.at[i], x_r.at[i], xpeer)

        return zc, zw, yc, yw, x_copy, x_wait

    def zback_z(k):
        return lax.rem(z + zs - k, zs)

    def azc(k, q):
        i = q * zs + k
        return rcopy(win.at[z, gh, q], win.at[z, gh, q], az_s.at[i], az_r.at[i], zfwd(k))

    def azw(k, q):
        s = win.at[zback_z(k), gh, q]
        i = q * zs + k
        return rcopy(s, s, az_s.at[i], az_r.at[i], zfwd(k))

    def axc(k, q):
        s = win.at[zback_z(k), gh, q]
        i = q * zs + k
        return rcopy(s, s, ax_s.at[i], ax_r.at[i], xpeer)

    def axw(k, q):
        s = win.at[zback_z(k), 1 - gh, q]
        i = q * zs + k
        return rcopy(s, s, ax_s.at[i], ax_r.at[i], xpeer)

    def each_piece(body):
        for q in range(pieces):
            loop(1, zs, lambda k: body(k, q))

    bzc, bzw, byc, byw, bxc, bxw = gather(wo, bz_s, bz_r, by_s, by_r, bx_s, bx_r)

    lc_in[0].wait()
    lc_in[1].wait()
    each_piece(lambda k, q: azc(k, q).start())
    lc_out[0].wait()
    lc_out[1].wait()
    byc(0).start()
    loop(1, zs, lambda k: bzc(k).start())

    e_up = rcopy(up_hbm.at[0], up.at[c], es.at[0], er.at[0], cpeer)
    e_down = rcopy(down_hbm.at[0], down.at[c], es.at[1], er.at[1], cpeer)
    e_up.start()
    e_down.start()
    lc_g.wait()

    def gcopy(d):
        return rcopy(gbuf.at[w], gbuf.at[w], gs.at[d], gr.at[d], {"wide": lax.rem(w + d, wide)})

    def gwait(d):
        s = gbuf.at[lax.rem(w + wide - d, wide)]
        return rcopy(s, s, gs.at[d], gr.at[d], {"wide": lax.rem(w + d, wide)})

    loop(1, wide, lambda d: gcopy(d).start())

    lc_tok.wait()
    step_rows = 32
    rin = nb.shape[4]

    def norm(i):
        rows = pl.ds(pl.multiple_of(i * step_rows, step_rows), step_rows)
        x = tok[rows, :].astype(F32)
        scale = lax.rsqrt(jnp.mean(x * x, axis=-1, keepdims=True) + 1e-05)
        n = (x * scale * gain_ref[...]).astype(BF16)
        part = i // (th // step_rows)
        within = pl.ds(pl.multiple_of(lax.rem(i, th // step_rows) * step_rows, step_rows), step_rows)
        for j in range(wide):
            nb[j % 2, part, j // 2, within, :] = n[:, j * rin : (j + 1) * rin]

    loop(0, tokens // step_rows, norm)

    tsend = rcopy(nb.at[oy, c], nby.at[c], ty_s, ty_r, ypeer)
    tsend.start()

    def madd(zz):
        wb = win[zz].reshape(2 * pieces * piece, lcols)
        for r in range(2):
            acc[r] += jnp.dot(nb[y, r, zz], wb, preferred_element_type=F32)
            acc[2 + r] += jnp.dot(nby[r, zz], wb, preferred_element_type=F32)

    acc[...] = jnp.zeros_like(acc)

    def z_arrive(k, q):
        azw(k, q).wait_recv()
        axc(k, q).start()

    each_piece(z_arrive)
    rcopy(nby.at[c], nby.at[c], ty_s, ty_r, ypeer).wait_recv()
    tfwd = rcopy(nby.at[c], nby.at[c], tc_s, tc_r, cpeer)
    tfwd.start()
    rcopy(nby.at[1 - c], nby.at[1 - c], tc_s, tc_r, cpeer).wait_recv()
    madd(z)

    def use_near(k):
        for q in range(pieces):
            axw(k, q).wait_recv()
        madd(zback_z(k))

    bzw(1).wait_recv()
    bxc(1, False).start()
    byc(1).start()
    loop(1, zs, use_near)
    psend[...] = acc[2:4].astype(BF16)
    pcopy = rcopy(psend, precv, py_s, py_r, ypeer)
    pcopy.start()
    pcopy.wait_recv()

    hrow = th // 2

    def lpiece(b, q, r):
        return lat.at[b, q, pl.ds(r * hrow, hrow)]

    def czc(k, q, r):
        s = lpiece(w, q, r)
        i = (q * 2 + r) * zs + k
        return rcopy(s, s, cz_s.at[i], cz_r.at[i], zfwd(k))

    def czw(k, q, r):
        s = lpiece(blk(k, y), q, r)
        i = (q * 2 + r) * zs + k
        return rcopy(s, s, cz_s.at[i], cz_r.at[i], zfwd(k))

    def cyc(k, q, r):
        s = lpiece(blk(k, y), q, r)
        i = (q * 2 + r) * zs + k
        return rcopy(s, s, cy_s.at[i], cy_r.at[i], ypeer)

    def cyw(k, q, r):
        s = lpiece(blk(k, oy), q, r)
        i = (q * 2 + r) * zs + k
        return rcopy(s, s, cy_s.at[i], cy_r.at[i], ypeer)

    xsend[...] = (acc[1 - c] + precv[1 - c].astype(F32)).astype(BF16)
    swap = rcopy(xsend, lat.at[w, c], cc_s, cc_r, cpeer)
    swap.start()
    lat[w, c] = (acc[c] + precv[c].astype(F32)).astype(BF16)
    for r in range(2):
        cyc(0, c, r).start()
        czc(1, c, r).start()
    rcopy(xsend, lat.at[w, 1 - c], cc_s, cc_r, cpeer).wait_recv()
    for r in range(2):
        cyc(0, 1 - c, r).start()
        czc(1, 1 - c, r).start()

    def later(k):
        for q in (c, 1 - c):
            for r in range(2):
                czc(k, q, r).start()

    loop(2, zs, later)

    lc_up.wait()
    lc_down.wait()
    rcopy(up_hbm.at[0], up.at[1 - c], es.at[0], er.at[0], cpeer).wait_recv()
    rcopy(down_hbm.at[0], down.at[1 - c], es.at[1], er.at[1], cpeer).wait_recv()
    loop(1, wide, lambda d: gwait(d).wait_recv())

    def gate_col(b):
        gt = gbuf[b]
        mine = lax.broadcasted_iota(jnp.int32, gt.shape, 0) == w
        row = jnp.sum(jnp.where(mine, gt, 0.0), axis=0, keepdims=True)
        return jnp.transpose(jnp.broadcast_to(row, (8, th)))[:, :1]

    hcol = ysend.shape[3]

    def dyc(k, q):
        i = q * zs + k
        return rcopy(ysend.at[k, q], yrecv.at[k, q], dy_s.at[i], dy_r.at[i], ypeer)

    def dzc(k, q):
        i = q * zs + k
        return rcopy(zsend.at[k, q], zrecv.at[k, q], dz_s.at[i], dz_r.at[i], zback(k))

    def expert(k):
        b0 = blk(k, 0)
        x0 = jnp.concatenate([lat[b0, 0], lat[b0 + 1, 0]], axis=0)
        x1 = jnp.concatenate([lat[b0, 1], lat[b0 + 1, 1]], axis=0)
        x = jnp.concatenate([x0, x1], axis=1)
        total = None
        for h in range(2):
            hid = lax.dot_general(x, up[h], (((1,), (1,)), ((), ())), preferred_element_type=F32)
            hid = jnp.square(jnp.maximum(hid, 0.0)).astype(BF16)
            part = jnp.dot(hid, down[h], preferred_element_type=F32)
            total = part if total is None else total + part
        obuf[0] = total[:th] * gate_col(b0)
        obuf[1] = total[th:] * gate_col(b0 + 1)
        for q in range(2):
            ysend[k, q] = obuf[oy, :, q * hcol : (q + 1) * hcol].astype(BF16)
            dyc(k, q).start()
        ownp[lax.rem(k, 2)] = obuf[y]

    def finish(k):
        for q in range(2):
            dyc(k, q).wait_recv()
            own = ownp[lax.rem(k, 2), :, q * hcol : (q + 1) * hcol]
            zsend[k, q] = (own + yrecv[k, q].astype(F32)).astype(BF16)
            dzc(k, q).start()

    order = [(q, r) for q in (c, 1 - c) for r in range(2)]

    def arrive(k, q, r):
        czw(k, q, r).wait_recv()
        cyc(k, q, r).start()

    def arrive_all(k):
        for q, r in order:
            arrive(k, q, r)

    def far_rows(k):
        for q, r in order:
            cyw(k, q, r).wait_recv()

    def b_arrive(k):
        bzw(k).wait_recv()
        bxc(k, False).start()
        byc(k).start()

    def by_arrive(k):
        byw(k).wait_recv()
        bxc(k, True).start()

    arrive_all(1)
    far_rows(0)
    expert(0)
    by_arrive(0)

    def expert_step(k):
        @pl.when(k < zs - 1)
        def _():
            arrive_all(k + 1)

        far_rows(k)
        expert(k)

        @pl.when(k > 1)
        def _():
            finish(k - 1)

        @pl.when(k == 1)
        def _():
            for q in range(2):
                dyc(0, q).wait_recv()
                cols = slice(q * hcol, (q + 1) * hcol)
                macc[:, cols] = ownp[0, :, cols] + yrecv[0, q].astype(F32)
            by_arrive(1)

        @pl.when((k > 1) & (k < zs - 1))
        def _():
            b_arrive(k)

    loop(1, zs, expert_step)
    loop(zs - 1, zs, b_arrive)
    finish(zs - 1)
    loop(2, zs, by_arrive)

    def collect(k):
        for q in range(2):
            dzc(k, q).wait_recv()
            macc[:, q * hcol : (q + 1) * hcol] += zrecv[k, q].astype(F32)

    loop(1, zs, collect)
    mixb[c] = macc[...].astype(BF16)
    mcopy = rcopy(mixb.at[c], mixb.at[c], mc_s, mc_r, cpeer)
    mcopy.start()
    rcopy(mixb.at[1 - c], mixb.at[1 - c], mc_s, mc_r, cpeer).wait_recv()
    loop(1, zs, lambda k: bxw(k, False).wait_recv())
    loop(0, zs, lambda k: bxw(k, True).wait_recv())

    ocols = out_ref.shape[1]
    width = min(512, ocols)

    def project(i):
        m = mixb[...].reshape(tokens, mixb.shape[2])
        off = pl.multiple_of(i * width, width)
        wv = wo[:, :, :, pl.ds(off, width)].reshape(mixb.shape[2], width)
        branch = jnp.dot(m, wv, preferred_element_type=F32)
        own = tok[:, pl.ds(pl.multiple_of(c * ocols + off, width), width)].astype(F32)
        out_ref[:, pl.ds(off, width)] = (own + branch).astype(out_ref.dtype)

    loop(0, ocols // width, project)

    loop(1, wide, lambda d: gcopy(d).wait_send())
    e_up.wait_send()
    e_down.wait_send()
    swap.wait_send()
    mcopy.wait_send()
    tsend.wait_send()
    tfwd.wait_send()
    pcopy.wait_send()
    each_piece(lambda k, q: azc(k, q).wait_send())
    each_piece(lambda k, q: axc(k, q).wait_send())
    loop(1, zs, lambda k: bzc(k).wait_send())
    loop(0, zs, lambda k: byc(k).wait_send())
    loop(1, zs, lambda k: bxc(k, False).wait_send())
    loop(0, zs, lambda k: bxc(k, True).wait_send())
    for q, r in order:
        loop(1, zs, lambda k: czc(k, q, r).wait_send())
        loop(0, zs, lambda k: cyc(k, q, r).wait_send())
    for q in range(2):
        loop(0, zs, lambda k: dyc(k, q).wait_send())
        loop(1, zs, lambda k: dzc(k, q).wait_send())


def local(tokens, norm_gain, w_in, w_out, w_up, w_down, expert_ids, gate_weights):
    wide = lax.axis_size("wide")
    zs = wide // 2
    rows, depth = tokens.shape
    half = rows // 2
    latent = w_in.shape[1]
    pieces = 4
    piece = w_in.shape[0] // (2 * pieces)
    ids = expert_ids.T
    chosen = ids[:, None, :] == jnp.arange(wide, dtype=jnp.int32)[None, :, None]
    gates = jnp.sum(jnp.where(chosen, gate_weights.T[:, None, :], 0.0), axis=0)
    gates = gates.reshape(wide, 2, half).transpose(1, 0, 2)
    any_ = pl.BlockSpec(memory_space=pl.ANY)
    vmem = pl.BlockSpec(memory_space=pltpu.VMEM)
    dma = pltpu.SemaphoreType.DMA
    hid = w_up.shape[2]
    cols = w_out.shape[1]
    V = pltpu.VMEM
    scratch = [
        V((rows, depth), BF16),
        V((2, 2, zs, half, depth // wide), BF16),
        V((2, zs, half, depth // wide), BF16),
        V((zs, 2, pieces, piece, latent // 2), BF16),
        V((wide, 2, w_out.shape[0] // 2, cols), BF16),
        V((2, hid, latent), BF16),
        V((2, hid, latent), BF16),
        V((wide, wide, half), F32),
        V((wide, 2, half, latent // 2), BF16),
        V((4, half, latent // 2), F32),
        V((2, half, latent // 2), BF16),
        V((2, half, latent // 2), BF16),
        V((half, latent // 2), BF16),
        V((2, half, latent), F32),
        V((2, half, latent), F32),
        V((zs, 2, half, latent // 2), BF16),
        V((zs, 2, half, latent // 2), BF16),
        V((zs, 2, half, latent // 2), BF16),
        V((zs, 2, half, latent // 2), BF16),
        V((half, latent), F32),
        V((2, half, latent), BF16),
        dma((8,)),
        dma((wide,)), dma((wide,)),
        dma((2,)), dma((2,)),
    ]
    scratch += [dma((pieces * zs,))] * 4 + [dma] * 6 + [dma((zs,))] * 4 + [dma((wide,))] * 2
    scratch += [dma((4 * zs,))] * 4 + [dma, dma] + [dma((2 * zs,))] * 4 + [dma, dma]
    return pl.pallas_call(
        kernel,
        out_shape=jax.ShapeDtypeStruct((rows, cols), BF16),
        in_specs=[any_, vmem, any_, any_, any_, any_, any_],
        out_specs=vmem,
        scratch_shapes=scratch,
        compiler_params=pltpu.CompilerParams(
            collective_id=0, has_side_effects=True, vmem_limit_bytes=66_000_000
        ),
        name="moe",
    )(tokens, norm_gain.reshape(1, depth), w_in.reshape(2, pieces, piece, latent), w_out, w_up.swapaxes(1, 2), w_down, gates)


def solution(mesh):
    in_specs = (
        P(("groups", "wide"), None),
        P(),
        P("wide", None),
        P("wide", "narrow"),
        P("wide", None, "narrow"),
        P("wide", "narrow", None),
        P(("groups", "wide"), None),
        P(("groups", "wide"), None),
    )
    out_specs = P(("groups", "wide"), "narrow")
    return jax.shard_map(local, mesh=mesh, in_specs=in_specs, out_specs=out_specs, check_vma=False)
```
